32 devices in a mesh: dp: 16 (over z, y, x), rep: 2 (over core).
Axes of the slice: x: 2, y: 2, z: 4, core: 2. Of those that a mesh axis runs over, the one named last changes fastest.
Arguments:
- ids: int32 [8192], P(('dp', 'rep')), may hold values from 0 to 65520
- counts: int32 [32], P(('dp', 'rep')), may hold values from 1 to 256, as said below
- hash_scale: int32 [512], replicated, may hold values from 1 to 32767
- hash_shift: int32 [512], replicated, may hold values from 0 to 65520
- w_code: bfloat16 [512, 1024], replicated, may hold values from -0.25 to 0.25
- norm_gain: float32 [1024], replicated, may hold values from 0.5 to 1.5
- norm_bias: float32 [1024], replicated, may hold values from -3 to 3
- w_out: bfloat16 [1024, 128], replicated, may hold values from -0.1875 to 0.1875
- out_bias: float32 [128], replicated, may hold values from -3 to 3
- cotangent: bfloat16 [8192, 128], P(('dp', 'rep')), may hold values from -6 to 6
Outputs:
- embeddings: bfloat16 [8192, 128], P(('dp', 'rep'))
- grad_code_t: float32 [1024, 512], P(('dp', 'rep'))
- grad_out: float32 [1024, 128], P(('dp', 'rep'))
- grad_gain: float32 [1024], replicated
- grad_bias: float32 [1024], replicated
The draws below stay inside these ranges and needn't reach their ends.
Inputs may be any that keep to these rules, and one draw needn't show every extreme that they name: Each device has 1 to 256 live slots, the first ones of its slots; the counts of the devices of one rep index sum to exactly 1024, and in each such group one device has exactly 256.
All inputs are finite; a program needn't handle non-finite values.
Results may differ from the reference program's by a relative error of at most 0.006.
Values may be sent and summed in bfloat16 or wider, within the bound.
No kernel may reach another device: no remote copies, remote signals or barrier semaphores. Data moves between devices by JAX's collectives and lax.ppermute only.
A program may use at most 64 MiB of HBM per device.

```python
import math
import jax
import jax.numpy as jnp
import numpy as np
from jax import lax

CODES = 512
HID = 1024
OUT = 128
SLOTS = 256
SLOTS_ALL = 8192
LIVE_GROUP = 1024
LIVE_ALL = 2048
N_DP = 16
N_REP = 2


def draw_counts(key, part):
    groups = []
    for member in range(N_REP):
        group_key = jax.random.fold_in(key, 7919 + member)
        key_base, key_peak, key_order = jax.random.split(group_key, 3)
        device_index = jnp.arange(N_DP, dtype=jnp.int32)
        base_weight = jax.random.randint(key_base, (N_DP,), 1, 3).astype(jnp.int32)
        ramp_weight = N_DP - 1 + 2 * device_index
        peak_index = jax.random.randint(key_peak, (), 0, N_DP).astype(jnp.int32)
        weight = jnp.where(device_index == peak_index, 0, base_weight * ramp_weight)
        surplus = LIVE_GROUP - SLOTS - (N_DP - 1)
        portion = surplus * weight // jnp.sum(weight)
        counts = jnp.where(device_index == peak_index, SLOTS, 1 + portion).astype(jnp.int32)
        remainder = LIVE_GROUP - jnp.sum(counts)
        priority = jnp.where(device_index == peak_index, N_DP, jax.random.permutation(key_order, N_DP).astype(jnp.int32))
        position = jnp.argsort(jnp.argsort(priority))
        counts = counts + (position < remainder).astype(jnp.int32)
        groups.append(counts)
    return jnp.stack(groups, axis=1).reshape(-1).astype(jnp.int32)


def touch_ends(values, rng, low, top_value):
    spot = [jax.random.randint(jax.random.fold_in(rng, axis), (), 0, length) for axis, length in enumerate(values.shape)]
    main_axis = values.shape.index(max(values.shape))
    beside = spot[:main_axis] + [(spot[main_axis] + 1) % values.shape[main_axis]] + spot[main_axis + 1:]
    return values.at[tuple(spot)].set(low).at[tuple(beside)].set(top_value)


def level_of(stream_key, extent, cuts, smallest, top_value):
    def one(dim, parts):
        draws = jax.random.uniform(jax.random.fold_in(jax.random.fold_in(stream_key, 6), dim), (parts,), jnp.float32, smallest / len(cuts), top_value / len(cuts))
        return jnp.repeat(jnp.exp(draws), extent[dim] // parts).reshape((-1,) + (1,) * (len(extent) - dim - 1))

    level = one(*cuts[0])
    for cut in cuts[1:]:
        level = level * one(*cut)
    return level


def rank_table(count, lean):
    loads = [(1 << 20) // math.isqrt(grade ** lean) + 1 for grade in range(1, count + 1)]
    scale = 1 + sum(loads) // (1 << 30)
    return np.cumsum(np.array([max(1, weight // scale) for weight in loads]))


def skewed_ids(key, shape, count, lean):
    grid = rank_table(count, lean)
    lot = jax.random.randint(jax.random.fold_in(key, 1), shape, 0, int(grid[count - 1]))
    grade = jnp.searchsorted(jnp.asarray(grid, jnp.int32), lot, side="right")
    return jax.random.permutation(jax.random.fold_in(key, 2), count)[grade].astype(jnp.int32)


def centred(rng, extent, scale, limit, shards=(), kind=jnp.bfloat16):
    values = jax.random.normal(rng, extent, jnp.float32) * scale
    if len(shards) > 0:
        values = level_of(rng, extent, shards, -0.22, 0.18) * values
    return jnp.clip(values, min=-limit, max=limit).astype(kind)


def setup_inputs(seed: int = 0) -> dict:
    key_list = jax.random.split(jax.random.key(seed), 11)
    return {
        "ids": touch_ends(skewed_ids(key_list[0], (SLOTS_ALL,), 65521, 2), jax.random.fold_in(key_list[0], 3), 0, 65520).astype(jnp.int32),
        "counts": draw_counts(jax.random.fold_in(key_list[10], 71), 0),
        "hash_scale": touch_ends(jax.random.randint(key_list[2], (CODES,), 1, 32768), jax.random.fold_in(key_list[2], 1), 1, 32767).astype(jnp.int32),
        "hash_shift": touch_ends(jax.random.randint(key_list[3], (CODES,), 0, 65521), jax.random.fold_in(key_list[3], 1), 0, 65520).astype(jnp.int32),
        "w_code": centred(key_list[4], (CODES, HID), CODES ** -0.5, 0.25),
        "norm_gain": jnp.clip(jax.random.uniform(key_list[5], (HID,), jnp.float32, 0.5, 1.5), 0.5, 1.5),
        "norm_bias": centred(key_list[6], (HID,), 0.5, 3.0, (), jnp.float32),
        "w_out": centred(key_list[7], (HID, OUT), HID ** -0.5, 0.1875),
        "out_bias": centred(key_list[8], (OUT,), 0.5, 3.0, (), jnp.float32),
        "cotangent": centred(key_list[9], (SLOTS_ALL, OUT), 1.0, 6.0, ((0, 32),)),
    }


modulus = 65521
epsilon = 1e-05

def hashed(ident, hash_scale, hash_shift):
    resid = ident % modulus
    bucket = (hash_scale[None, :] * resid[:, None] + hash_shift[None, :]) % modulus
    return (bucket.astype(jnp.float32) * (2.0 / (modulus - 1)) - 1.0).astype(jnp.bfloat16)

def mish_parts(gated):
    softer = jax.nn.softplus(gated)
    tangent = jnp.tanh(softer)
    return (gated * tangent, tangent + gated * (1.0 - tangent * tangent) * jax.nn.sigmoid(gated))

def reference(ids, counts, hash_scale, hash_shift, w_code, norm_gain, norm_bias, w_out, out_bias, cotangent):
    width = w_out.shape[1]
    hidden = w_code.shape[1]
    owner_device = jnp.arange(SLOTS_ALL, dtype=jnp.int32) // SLOTS
    slot_index = jnp.arange(SLOTS_ALL, dtype=jnp.int32) % SLOTS
    is_live = slot_index < counts[owner_device]
    live_order = jnp.argsort(jnp.where(is_live, 0, 1).astype(jnp.int32), stable=True)[:LIVE_ALL]
    group_count = LIVE_ALL // 1024
    sel_ids = ids[live_order].reshape(group_count, 1024)
    sel_cot = cotangent[live_order].reshape(group_count, 1024, width)
    total = jnp.sum(counts).astype(jnp.float32)

    def forward(ident):
        code_rows = hashed(ident, hash_scale, hash_shift)
        return (code_rows, jnp.dot(code_rows, w_code, preferred_element_type=jnp.float32))

    def stats(state_carry, ident):
        preact = forward(ident)[1]
        return ((state_carry[0] + preact.sum(0), state_carry[1] + (preact * preact).sum(0)), None)
    zero_row = jnp.zeros((hidden,), jnp.float32)
    (sum_hidden, sum_square), _ = lax.scan(stats, (zero_row, zero_row), sel_ids)
    feature_mean = sum_hidden / total
    inv_std = lax.rsqrt(sum_square / total - feature_mean * feature_mean + epsilon)
    loss_scale = lax.rsqrt(total)

    def middle(ident, cot_rows):
        code_rows, preact = forward(ident)
        normed = (preact - feature_mean) * inv_std
        act_full, mish_slope = mish_parts(normed * norm_gain + norm_bias)
        activation = act_full.astype(jnp.bfloat16)
        delta_rows = (cot_rows.astype(jnp.float32) * loss_scale).astype(jnp.bfloat16)
        grad_act = lax.dot_general(delta_rows, w_out, (((1,), (1,)), ((), ())), preferred_element_type=jnp.float32)
        return (code_rows, normed, activation, delta_rows, grad_act * mish_slope)

    def second(state_carry, pair):
        code_rows, normed, activation, delta_rows, dvalue = middle(pair[0], pair[1])
        embedded = (jnp.dot(activation, w_out, preferred_element_type=jnp.float32) + out_bias).astype(jnp.bfloat16)
        out_part = lax.dot_general(activation, delta_rows, (((0,), (0,)), ((), ())), preferred_element_type=jnp.float32)
        return ((state_carry[0] + (dvalue * normed).sum(0), state_carry[1] + dvalue.sum(0), state_carry[2] + out_part), embedded)
    start_out = jnp.zeros((hidden, width), jnp.float32)
    (grad_gain, grad_bias, grad_out), embedded = lax.scan(second, (zero_row, zero_row, start_out), (sel_ids, sel_cot))

    def third(state_carry, pair):
        code_rows, normed, activation, delta_rows, dvalue = middle(pair[0], pair[1])
        dpre = (norm_gain * inv_std * (dvalue - grad_bias / total - normed * grad_gain / total)).astype(jnp.bfloat16)
        return (state_carry + lax.dot_general(dpre, code_rows, (((0,), (0,)), ((), ())), preferred_element_type=jnp.float32), None)
    grad_code_t, _ = lax.scan(third, jnp.zeros((hidden, w_code.shape[0]), jnp.float32), (sel_ids, sel_cot))
    embeddings = jnp.zeros((SLOTS_ALL, width), jnp.bfloat16).at[live_order].set(embedded.reshape(LIVE_ALL, width))
    return (embeddings, grad_code_t, grad_out, grad_gain, grad_bias)
```

```python
import math

import jax
import jax.numpy as jnp
from jax import lax
from jax.sharding import PartitionSpec as P

LANES = 128
modulus = 65521
epsilon = 1e-05
AXES = ("dp", "rep")


def hashed(ident, hash_scale, hash_shift):
    resid = ident % modulus
    bucket = (hash_scale[None, :] * resid[:, None] + hash_shift[None, :]) % modulus
    return (bucket.astype(jnp.float32) * (2.0 / (modulus - 1)) - 1.0).astype(jnp.bfloat16)


def mish_parts(gated):
    softer = jax.nn.softplus(gated)
    tangent = jnp.tanh(softer)
    return (gated * tangent, tangent + gated * (1.0 - tangent * tangent) * jax.nn.sigmoid(gated))


def exchange(blocks):
    return lax.all_to_all(blocks, AXES, split_axis=0, concat_axis=0, tiled=True)


def lane_rows(flat):
    pad = -flat.shape[-1] % (8 * LANES)
    flat = jnp.pad(flat, [(0, 0)] * (flat.ndim - 1) + [(0, pad)])
    return flat.reshape(flat.shape[:-1] + (-1, LANES))


def per_device(
    ids, counts, hash_scale, hash_shift, w_code, norm_gain, norm_bias, w_out, out_bias, cotangent
):
    devices = lax.axis_size("dp") * lax.axis_size("rep")
    me = lax.axis_index("dp") * lax.axis_size("rep") + lax.axis_index("rep")
    slots = ids.shape[0]
    codes, hidden = w_code.shape
    width = w_out.shape[1]
    share = hidden // devices
    keep = (jnp.arange(slots, dtype=jnp.int32) < counts[0])[:, None]

    preact = jnp.dot(
        hashed(ids, hash_scale, hash_shift), w_code, preferred_element_type=jnp.float32
    )
    masked = jnp.where(keep, preact, 0.0)
    row = lane_rows(
        jnp.concatenate(
            [
                masked.sum(0),
                (masked * masked).sum(0),
                ids.astype(jnp.float32),
                counts.astype(jnp.float32),
            ]
        )
    )
    table = exchange(jnp.broadcast_to(row, (devices,) + row.shape)).reshape(devices, -1)
    sums = table[:, : 2 * hidden].sum(0)
    all_ids = table[:, 2 * hidden : 2 * hidden + slots].astype(jnp.int32)
    all_counts = table[:, 2 * hidden + slots].astype(jnp.int32)
    total = all_counts.sum().astype(jnp.float32)
    mean = sums[:hidden] / total
    inv_std = lax.rsqrt(sums[hidden:] / total - mean * mean + epsilon)

    normed = (preact - mean) * inv_std
    act_full, slope = mish_parts(normed * norm_gain + norm_bias)
    act = act_full.astype(jnp.bfloat16)
    delta = jnp.where(keep, cotangent.astype(jnp.float32) * lax.rsqrt(total), 0.0).astype(
        jnp.bfloat16
    )
    dval = (
        lax.dot_general(delta, w_out, (((1,), (1,)), ((), ())), preferred_element_type=jnp.float32)
        * slope
    )
    grad_out = lax.dot_general(
        act, delta, (((0,), (0,)), ((), ())), preferred_element_type=jnp.float32
    )
    columns = exchange(dval.astype(jnp.bfloat16).T.reshape(devices, share, slots))
    pair = jnp.concatenate([(dval * normed).sum(0), dval.sum(0)])
    grads = exchange(
        lane_rows(
            jnp.concatenate(
                [
                    grad_out.reshape(devices, share * width),
                    jnp.broadcast_to(pair, (devices, 2 * hidden)),
                ],
                axis=1,
            )
        )
    )
    grads = grads.reshape(devices, -1)[:, : share * width + 2 * hidden].sum(0)
    out_share = grads[: share * width].reshape(share, width)
    grad_gain = grads[share * width : share * width + hidden]
    grad_bias = grads[share * width + hidden :]

    embedded = jnp.dot(act, w_out, preferred_element_type=jnp.float32) + out_bias
    embedded = jnp.where(keep, embedded, 0.0).astype(jnp.bfloat16)

    def own(vector):
        return lax.dynamic_slice_in_dim(vector, me * share, share, vector.ndim - 1)

    w_own = own(w_code)
    mean_own, inv_own = own(mean), own(inv_std)
    shift_own, tilt_own = own(grad_bias) / total, own(grad_gain) / total
    scale_own = own(norm_gain) * inv_own
    group = math.gcd(devices, max(1, 8192 // slots))

    def accumulate(index, grad_rows):
        start = index * group
        block_ids = lax.dynamic_slice_in_dim(all_ids, start, group, 0).reshape(-1)
        block_counts = lax.dynamic_slice_in_dim(all_counts, start, group, 0)
        block = lax.dynamic_slice_in_dim(columns, start, group, 0)
        code = hashed(block_ids, hash_scale, hash_shift)
        pre = lax.dot_general(
            w_own, code, (((0,), (1,)), ((), ())), preferred_element_type=jnp.float32
        )
        seen = (pre - mean_own[:, None]) * inv_own[:, None]
        dval_own = block.transpose(1, 0, 2).reshape(share, -1).astype(jnp.float32)
        dpre = scale_own[:, None] * (dval_own - shift_own[:, None] - seen * tilt_own[:, None])
        live = jnp.arange(slots, dtype=jnp.int32)[None, :] < block_counts[:, None]
        dpre = jnp.where(live.reshape(1, -1), dpre, 0.0).astype(jnp.bfloat16)
        return grad_rows + jnp.dot(dpre, code, preferred_element_type=jnp.float32)

    code_share = lax.fori_loop(
        0, devices // group, accumulate, jnp.zeros((share, codes), jnp.float32)
    )
    return embedded, code_share, out_share, grad_gain, grad_bias


def solution(mesh):
    rows = P(AXES)
    return jax.shard_map(
        per_device,
        mesh=mesh,
        in_specs=(rows, rows, P(), P(), P(), P(), P(), P(), P(), P(AXES, None)),
        out_specs=(P(AXES, None), P(AXES, None), P(AXES, None), P(), P()),
        check_vma=False,
    )
```

```python
import functools
import math

import jax
import jax.numpy as jnp
from jax import lax
from jax.experimental import pallas as pl
from jax.experimental.pallas import tpu as pltpu
from jax.sharding import PartitionSpec as P

LANES = 128
modulus = 65521
epsilon = 1e-05
AXES = ("dp", "rep")


def hashed(ident, hash_scale, hash_shift):
    resid = ident % modulus
    bucket = (hash_scale[None, :] * resid[:, None] + hash_shift[None, :]) % modulus
    return (bucket.astype(jnp.float32) * (2.0 / (modulus - 1)) - 1.0).astype(jnp.bfloat16)


def mish_parts(gated):
    softer = jax.nn.softplus(gated)
    tangent = jnp.tanh(softer)
    return (gated * tangent, tangent + gated * (1.0 - tangent * tangent) * jax.nn.sigmoid(gated))


def exchange(blocks):
    return lax.all_to_all(blocks, AXES, split_axis=0, concat_axis=0, tiled=True)


def lane_rows(flat):
    pad = -flat.shape[-1] % (8 * LANES)
    flat = jnp.pad(flat, [(0, 0)] * (flat.ndim - 1) + [(0, pad)])
    return flat.reshape(flat.shape[:-1] + (-1, LANES))


def general_device(
    ids, counts, hash_scale, hash_shift, w_code, norm_gain, norm_bias, w_out, out_bias, cotangent
):
    devices = lax.axis_size("dp") * lax.axis_size("rep")
    me = lax.axis_index("dp") * lax.axis_size("rep") + lax.axis_index("rep")
    slots = ids.shape[0]
    codes, hidden = w_code.shape
    width = w_out.shape[1]
    share = hidden // devices
    keep = (jnp.arange(slots, dtype=jnp.int32) < counts[0])[:, None]

    preact = jnp.dot(
        hashed(ids, hash_scale, hash_shift), w_code, preferred_element_type=jnp.float32
    )
    masked = jnp.where(keep, preact, 0.0)
    row = lane_rows(
        jnp.concatenate(
            [
                masked.sum(0),
                (masked * masked).sum(0),
                ids.astype(jnp.float32),
                counts.astype(jnp.float32),
            ]
        )
    )
    table = exchange(jnp.broadcast_to(row, (devices,) + row.shape)).reshape(devices, -1)
    sums = table[:, : 2 * hidden].sum(0)
    all_ids = table[:, 2 * hidden : 2 * hidden + slots].astype(jnp.int32)
    all_counts = table[:, 2 * hidden + slots].astype(jnp.int32)
    total = all_counts.sum().astype(jnp.float32)
    mean = sums[:hidden] / total
    inv_std = lax.rsqrt(sums[hidden:] / total - mean * mean + epsilon)

    normed = (preact - mean) * inv_std
    act_full, slope = mish_parts(normed * norm_gain + norm_bias)
    act = act_full.astype(jnp.bfloat16)
    delta = jnp.where(keep, cotangent.astype(jnp.float32) * lax.rsqrt(total), 0.0).astype(
        jnp.bfloat16
    )
    dval = (
        lax.dot_general(delta, w_out, (((1,), (1,)), ((), ())), preferred_element_type=jnp.float32)
        * slope
    )
    grad_out = lax.dot_general(
        act, delta, (((0,), (0,)), ((), ())), preferred_element_type=jnp.float32
    )
    columns = exchange(dval.astype(jnp.bfloat16).T.reshape(devices, share, slots))
    pair = jnp.concatenate([(dval * normed).sum(0), dval.sum(0)])
    grads = exchange(
        lane_rows(
            jnp.concatenate(
                [
                    grad_out.reshape(devices, share * width),
                    jnp.broadcast_to(pair, (devices, 2 * hidden)),
                ],
                axis=1,
            )
        )
    )
    grads = grads.reshape(devices, -1)[:, : share * width + 2 * hidden].sum(0)
    out_share = grads[: share * width].reshape(share, width)
    grad_gain = grads[share * width : share * width + hidden]
    grad_bias = grads[share * width + hidden :]

    embedded = jnp.dot(act, w_out, preferred_element_type=jnp.float32) + out_bias
    embedded = jnp.where(keep, embedded, 0.0).astype(jnp.bfloat16)

    def own(vector):
        return lax.dynamic_slice_in_dim(vector, me * share, share, vector.ndim - 1)

    w_own = own(w_code)
    mean_own, inv_own = own(mean), own(inv_std)
    shift_own, tilt_own = own(grad_bias) / total, own(grad_gain) / total
    scale_own = own(norm_gain) * inv_own
    group = math.gcd(devices, max(1, 8192 // slots))

    def accumulate(index, grad_rows):
        start = index * group
        block_ids = lax.dynamic_slice_in_dim(all_ids, start, group, 0).reshape(-1)
        block_counts = lax.dynamic_slice_in_dim(all_counts, start, group, 0)
        block = lax.dynamic_slice_in_dim(columns, start, group, 0)
        code = hashed(block_ids, hash_scale, hash_shift)
        pre = lax.dot_general(
            w_own, code, (((0,), (1,)), ((), ())), preferred_element_type=jnp.float32
        )
        seen = (pre - mean_own[:, None]) * inv_own[:, None]
        dval_own = block.transpose(1, 0, 2).reshape(share, -1).astype(jnp.float32)
        dpre = scale_own[:, None] * (dval_own - shift_own[:, None] - seen * tilt_own[:, None])
        live = jnp.arange(slots, dtype=jnp.int32)[None, :] < block_counts[:, None]
        dpre = jnp.where(live.reshape(1, -1), dpre, 0.0).astype(jnp.bfloat16)
        return grad_rows + jnp.dot(dpre, code, preferred_element_type=jnp.float32)

    code_share = lax.fori_loop(
        0, devices // group, accumulate, jnp.zeros((share, codes), jnp.float32)
    )
    return embedded, code_share, out_share, grad_gain, grad_bias


def row_of(tiles):
    return jnp.concatenate(tiles, axis=1)


def place_block(tile, source, target, block):
    shift = ((target - source) * block) % LANES
    return pltpu.roll(tile, shift, 1) if shift else tile


def pick_blocks(x, chosen, block):
    per_tile = LANES // block
    lane = lax.broadcasted_iota(jnp.int32, (x.shape[0], LANES), 1) // block
    tiles = []
    for first in range(0, len(chosen), per_tile):
        tile = None
        for place, b in enumerate(chosen[first : first + per_tile]):
            start = b // per_tile * LANES
            piece = place_block(x[:, start : start + LANES], b % per_tile, place, block)
            tile = piece if tile is None else jnp.where(lane == place, piece, tile)
        tiles.append(tile)
    return tiles


def split_pair(x):
    high = x.astype(jnp.bfloat16).astype(jnp.float32)
    return high, (x - high).astype(jnp.bfloat16).astype(jnp.float32)


def codes_of(id_column, scale_row, shift_row):
    raw = scale_row * id_column + shift_row
    once = lax.shift_right_logical(raw, 16) * 15 + lax.bitwise_and(raw, 65535)
    twice = lax.shift_right_logical(once, 16) * 15 + lax.bitwise_and(once, 65535)
    bucket = jnp.where(twice >= modulus, twice - modulus, twice)
    return (bucket.astype(jnp.float32) * (2.0 / (modulus - 1)) - 1.0).astype(jnp.bfloat16)


def mish_of(val):
    grown = jnp.exp(jnp.minimum(val, 20.0))
    n = grown * (grown + 2.0)
    inverse = 1.0 / (n + 2.0)
    t = n * inverse
    slope = t + val * (4.0 * grown * (1.0 + grown)) * (inverse * inverse)
    return val * t, slope


def dot_t(a, b):
    return lax.dot_general(a, b, (((1,), (1,)), ((), ())), preferred_element_type=jnp.float32)


def dot_rows(a, b):
    return lax.dot_general(a, b, (((0,), (0,)), ((), ())), preferred_element_type=jnp.float32)


def one_hot(condition):
    return jnp.where(condition, 1.0, 0.0).astype(jnp.bfloat16)


def first_kernel(dims, count_ref, ids_ref, scale_ref, shift_ref, w_ref, cot_ref, send_ref, pre_ref):
    chips, reps, take, block = dims.chips, dims.reps, dims.take, dims.block
    slots = dims.slots
    count = count_ref[0]
    resid = lax.rem(ids_ref[...], modulus)
    high = lax.shift_right_logical(resid, 8).astype(jnp.float32)
    low = lax.bitwise_and(resid, 255).astype(jnp.float32)
    r = lax.broadcasted_iota(jnp.int32, (slots, slots), 0)
    c = lax.broadcasted_iota(jnp.int32, (slots, slots), 1)
    blank = jnp.zeros((6, slots), jnp.float32)
    pieces = jnp.concatenate([high, low, blank], axis=0).astype(jnp.bfloat16)
    columns = dot_t(one_hot(r == c), pieces)
    id_column = (columns[:, 0:1] * 256.0 + columns[:, 1:2]).astype(jnp.int32)
    codes = codes_of(id_column, scale_ref[...], shift_ref[...])
    pre = jnp.dot(codes, w_ref[...], preferred_element_type=jnp.float32)
    pre_ref[...] = pre
    keep = lax.broadcasted_iota(jnp.int32, (slots, 1), 0) < count
    sums = jnp.where(keep, pre, 0.0).sum(0, keepdims=True)
    apart = jnp.where(keep, pre - sums / count.astype(jnp.float32), 0.0)
    spread = (apart * apart).sum(0, keepdims=True)
    stats = jnp.concatenate(split_pair(sums) + split_pair(spread), axis=0)
    order = one_hot(c == (r % take) * chips + r // take)
    moved = jnp.dot(order, cot_ref[...], preferred_element_type=jnp.float32).astype(jnp.bfloat16)
    by_chip = dot_t(pieces, order)
    lane_parts = slots // LANES
    tail = [by_chip[i : i + 1, t * LANES : (t + 1) * LANES] for i in range(2) for t in range(lane_parts)]
    tail.append(jnp.full((1, LANES), 1.0, jnp.float32) * count.astype(jnp.float32))
    tail.append(jnp.zeros((dims.send_rows - take - dims.stat_rows - len(tail), LANES), jnp.float32))
    tail = jnp.concatenate(tail, axis=0)
    for rep in range(reps):
        tiles = pick_blocks(stats, [k * reps + rep for k in range(chips)], block)
        lower = jnp.concatenate(tiles + [tail], axis=0).astype(jnp.bfloat16)
        for k in range(chips):
            send_ref[k * reps + rep, :take, :] = moved[k * take : (k + 1) * take, :]
            send_ref[k * reps + rep, take:, :] = lower


def count_column(dims, recv):
    row = dims.take + dims.stat_rows + 2 * (dims.slots // LANES)
    return recv[:, row, :][:, 0:1]


def id_table(dims, recv):
    base = dims.take + dims.stat_rows
    parts = dims.slots // LANES
    rows = dims.devices * dims.take
    spread = one_hot(
        lax.broadcasted_iota(jnp.int32, (rows, dims.devices), 0) // dims.take
        == lax.broadcasted_iota(jnp.int32, (rows, dims.devices), 1)
    )
    own_j = (
        lax.broadcasted_iota(jnp.int32, (rows, dims.slots), 1) % dims.take
        == lax.broadcasted_iota(jnp.int32, (rows, dims.slots), 0) % dims.take
    )
    fold = one_hot(
        lax.broadcasted_iota(jnp.int32, (dims.slots, LANES), 0) // dims.take
        == lax.broadcasted_iota(jnp.int32, (dims.slots, LANES), 1)
    )
    tables = []
    for i in range(2):
        flat = row_of([recv[:, base + i * parts + t, :] for t in range(parts)]).astype(jnp.bfloat16)
        wide = jnp.dot(spread, flat, preferred_element_type=jnp.float32)
        wide = jnp.where(own_j, wide, 0.0).astype(jnp.bfloat16)
        tables.append(jnp.dot(wide, fold, preferred_element_type=jnp.float32).astype(jnp.bfloat16))
    return tables


def packing(dims, counts, chip):
    lanes = dims.devices * dims.take
    d = lax.broadcasted_iota(jnp.int32, (dims.devices, lanes), 0)
    l = lax.broadcasted_iota(jnp.int32, (dims.devices, lanes), 1) // dims.take
    j = (lax.broadcasted_iota(jnp.int32, (1, lanes), 1) % dims.take).astype(jnp.float32)
    chip = chip.astype(jnp.float32) if hasattr(chip, "astype") else float(chip)
    live = jnp.maximum(jnp.floor((counts - chip + (dims.chips - 1.0)) * (1.0 / dims.chips)), 0.0)
    before = jnp.where(d < l, live, 0.0).sum(0, keepdims=True)
    here = jnp.where(d == l, live, 0.0).sum(0, keepdims=True)
    target = jnp.where(j < here, before + j, -1.0).astype(jnp.int32)
    row = lax.broadcasted_iota(jnp.int32, (dims.rows, lanes), 0)
    return one_hot(row == target), live.sum(0, keepdims=True)


def middle_kernel(
    dims, place_ref, recv_ref, w_ref, gain_ref, bias_ref, w_out_ref, scale_ref, shift_ref,
    send_ref, stat_ref,
):
    take, block, rows = dims.take, dims.block, dims.rows
    half, groups = dims.half, dims.groups
    chip = place_ref[0]
    recv = recv_ref[...].astype(jnp.float32)
    counts = count_column(dims, recv)
    total = counts.sum(0, keepdims=True)
    means, variances = [], []
    for t in range(half // LANES):
        r = take + 4 * t
        sums = recv[:, r, :] + recv[:, r + 1, :]
        spread = recv[:, r + 2, :] + recv[:, r + 3, :]
        mean = sums.sum(0, keepdims=True) / total
        off = sums / counts - mean
        means.append(mean)
        variances.append((spread + counts * (off * off)).sum(0, keepdims=True) / total)
    mean = row_of(means)
    inv_std = lax.rsqrt(row_of(variances) + epsilon)
    stat_ref[...] = jnp.concatenate([mean, inv_std, jnp.zeros((6, half), jnp.float32)], axis=0)

    pack, _ = packing(dims, counts, chip)
    cot = jnp.dot(
        pack, recv_ref[:, :take, :].reshape(dims.devices * take, LANES),
        preferred_element_type=jnp.float32,
    )
    high, low = id_table(dims, recv)
    lane = lax.broadcasted_iota(jnp.int32, (rows, LANES), 1)
    ids = jnp.dot(pack, high, preferred_element_type=jnp.float32) * 256.0 + jnp.dot(
        pack, low, preferred_element_type=jnp.float32
    )
    id_column = jnp.where(lane == chip, ids, 0.0).sum(1, keepdims=True).astype(jnp.int32)
    codes = codes_of(id_column, scale_ref[...], shift_ref[...])
    pre = jnp.dot(codes, w_ref[...], preferred_element_type=jnp.float32)
    normed = (pre - mean) * inv_std
    act, slope = mish_of(normed * gain_ref[...] + bias_ref[...])
    delta = (cot * lax.rsqrt(total)).astype(jnp.bfloat16)
    dval = dot_t(delta, w_out_ref[...]) * slope
    grad_out = dot_rows(act.astype(jnp.bfloat16), delta).astype(jnp.bfloat16)
    gain_pair = split_pair((dval * normed).sum(0, keepdims=True))
    bias_pair = split_pair(dval.sum(0, keepdims=True))
    four = jnp.concatenate(gain_pair + bias_pair, axis=0)
    four = jnp.concatenate(
        [four[:, t * LANES : (t + 1) * LANES] for t in range(half // LANES)], axis=0
    ).astype(jnp.bfloat16)
    part = rows // groups
    lane = lax.broadcasted_iota(jnp.int32, (part, LANES), 1) // block
    for k in range(dims.chips):
        start = k // groups * LANES
        tile = None
        for q in range(groups):
            piece = dval[q * part : (q + 1) * part, start : start + LANES]
            piece = place_block(piece, k % groups, q, block)
            tile = piece if tile is None else jnp.where(lane == q, piece, tile)
        send_ref[k, :part, :] = tile.astype(jnp.bfloat16)
        send_ref[k, part : part + block, :] = grad_out[k * block : (k + 1) * block, :]
        send_ref[k, part + block :, :] = four


def embed_kernel(
    dims, count_ref, total_ref, pre_ref, mean_ref, inv_ref, gain_ref, bias_ref, w_out_ref,
    out_bias_ref, out_ref,
):
    normed = (pre_ref[...] - mean_ref[...]) * inv_ref[...]
    act, _ = mish_of(normed * gain_ref[...] + bias_ref[...])
    out = jnp.dot(act.astype(jnp.bfloat16), w_out_ref[...], preferred_element_type=jnp.float32)
    keep = lax.broadcasted_iota(jnp.int32, (dims.slots, 1), 0) < count_ref[0]
    out_ref[...] = jnp.where(keep, out + out_bias_ref[...], 0.0).astype(jnp.bfloat16)


def owner_kernel(dims, recv_ref, w_ref, scale_ref, shift_ref, code_ref, pre_ref, live_ref):
    recv = recv_ref[...].astype(jnp.float32)
    counts = count_column(dims, recv)
    part = dims.rows // dims.groups
    tables = id_table(dims, recv)
    both = row_of([table.astype(jnp.float32) for table in tables]).astype(jnp.bfloat16)
    row = lax.broadcasted_iota(jnp.int32, (part, LANES), 0)
    group = lax.broadcasted_iota(jnp.int32, (part, LANES), 1) // dims.block
    for s in range(dims.chips):
        pack, live = packing(dims, counts, s)
        ids = jnp.dot(pack, both, preferred_element_type=jnp.float32)
        id_column = (ids[:, s : s + 1] * 256.0 + ids[:, LANES + s : LANES + s + 1]).astype(jnp.int32)
        codes = codes_of(id_column, scale_ref[...], shift_ref[...])
        rows = pl.ds(s * part, part)
        pre = None
        for q in range(dims.groups):
            chunk = codes[q * part : (q + 1) * part, :]
            code_ref[q, rows, :] = chunk
            term = jnp.dot(chunk, w_ref[q], preferred_element_type=jnp.float32)
            pre = term if pre is None else pre + term
        pre_ref[rows, :] = pre
        live_ref[rows, :] = jnp.where(
            (group * part + row).astype(jnp.float32) < live, 1.0, 0.0
        )


def spread_own(dims, x, chip):
    groups, block = dims.groups, dims.block
    lane = lax.broadcasted_iota(jnp.int32, (1, LANES), 1) // block
    own = jnp.zeros((1, LANES), jnp.float32)
    for t in range(dims.half // LANES):
        own = own + jnp.where(
            lane + t * groups == chip, x[:, t * LANES : (t + 1) * LANES], 0.0
        )
    out = own
    for i in range(1, groups):
        out = out + pltpu.roll(own, i * block, 1)
    return out


def last_kernel(
    dims, place_ref, total_ref, recv_ref, code_ref, pre_ref, live_ref, stat_ref, gain_ref,
    code_out_ref, out_out_ref, pair_ref,
):
    part, block, groups = dims.rows // dims.groups, dims.block, dims.groups
    chip = place_ref[0]
    total = total_ref[0].astype(jnp.float32)
    four = recv_ref[:, part + block :, :].astype(jnp.float32).sum(0)
    gains, biases = [], []
    for t in range(dims.half // LANES):
        gains.append(four[4 * t : 4 * t + 1, :] + four[4 * t + 1 : 4 * t + 2, :])
        biases.append(four[4 * t + 2 : 4 * t + 3, :] + four[4 * t + 3 : 4 * t + 4, :])
    gain, bias = row_of(gains), row_of(biases)
    pair_ref[...] = jnp.concatenate([gain, bias, jnp.zeros((6, dims.half), jnp.float32)], axis=0)
    out_out_ref[...] = recv_ref[:, part : part + block, :].astype(jnp.float32).sum(0)
    mean = spread_own(dims, stat_ref[0:1, :], chip)
    inv_std = spread_own(dims, stat_ref[1:2, :], chip)
    scale = spread_own(dims, gain_ref[...], chip) * inv_std
    shift = spread_own(dims, bias, chip) / total
    tilt = spread_own(dims, gain, chip) / total
    dval = recv_ref[:, :part, :].astype(jnp.float32).reshape(dims.chips * part, LANES)
    normed = (pre_ref[...] - mean) * inv_std
    dpre = scale * (dval - shift - normed * tilt)
    dpre = jnp.where(live_ref[...] > 0.5, dpre, 0.0).astype(jnp.bfloat16)
    out = None
    for q in range(groups):
        term = dot_rows(dpre, code_ref[q])[q * block : (q + 1) * block, :]
        out = term if out is None else out + term
    code_out_ref[...] = out


class Dims:
    def __init__(self, mesh, slots, codes, hidden, width):
        self.chips, self.reps = mesh.shape["dp"], mesh.shape["rep"]
        self.devices = self.chips * self.reps
        self.slots, self.codes, self.hidden, self.width = slots, codes, hidden, width
        self.block = hidden // self.devices
        self.half = hidden // self.reps
        self.groups = LANES // max(1, self.block)
        self.take = slots // self.chips
        bound = self.devices * slots // 4 // self.chips
        bound += self.devices * (self.chips - 1) // self.chips
        step = 8 * self.groups
        self.rows = min(-(-bound // step) * step, self.devices * self.take)
        self.stat_rows = 4 * self.half // LANES
        self.send_rows = -(-(self.take + self.stat_rows + 2 * slots // LANES + 1) // 8) * 8
        self.grad_rows = self.rows // self.groups + self.block + self.stat_rows
        self.vmem = 48 << 20

    def fits(self):
        return (
            self.width == LANES
            and LANES % self.block == 0
            and self.block % 8 == 0
            and self.take % 8 == 0
            and self.slots % LANES == 0
            and self.half % LANES == 0
            and self.codes % LANES == 0
            and self.chips <= LANES
            and self.slots <= 256
            and self.rows % (8 * self.groups) == 0
            and self.chips * self.rows * self.codes <= (1 << 22)
        )


def kernel_call(dims, body, outs, arguments, scalars, name, flops):
    specs = [pl.BlockSpec(memory_space=pltpu.SMEM)] * scalars
    specs += [pl.BlockSpec(memory_space=pltpu.VMEM)] * (len(arguments) - scalars)
    return pl.pallas_call(
        functools.partial(body, dims),
        out_shape=[jax.ShapeDtypeStruct(shape, kind) for shape, kind in outs],
        in_specs=specs,
        out_specs=[pl.BlockSpec(memory_space=pltpu.VMEM)] * len(outs),
        compiler_params=pltpu.CompilerParams(vmem_limit_bytes=dims.vmem),
        cost_estimate=pl.CostEstimate(flops=flops, bytes_accessed=1 << 20, transcendentals=0),
        name=name,
    )(*arguments)


def fast_device(
    dims, ids, counts, hash_scale, hash_shift, w_code, norm_gain, norm_bias, w_out, out_bias,
    cotangent,
):
    chips, reps, block, half = dims.chips, dims.reps, dims.block, dims.half
    dp, rep = lax.axis_index("dp"), lax.axis_index("rep")
    f32, bf16 = jnp.float32, jnp.bfloat16
    scale_row, shift_row = hash_scale.reshape(1, -1), hash_shift.reshape(1, -1)
    send, pre = kernel_call(
        dims, first_kernel,
        [((dims.devices, dims.send_rows, LANES), bf16), ((dims.slots, dims.hidden), f32)],
        (counts, ids.reshape(1, -1), scale_row, shift_row, w_code, cotangent), 1, "first", 10**9,
    )
    recv = exchange(send)

    def of_rep(x, axis):
        shape = x.shape[:axis] + (chips, reps, block) + x.shape[axis + 1 :]
        x = lax.dynamic_index_in_dim(x.reshape(shape), rep, axis + 1, keepdims=False)
        return x.reshape(x.shape[:axis] + (half,) + x.shape[axis + 2 :])

    place = dp.reshape(1).astype(jnp.int32)
    w_half, w_out_half = of_rep(w_code, 1), of_rep(w_out, 0)
    gain_half = of_rep(norm_gain, 0).reshape(1, -1)
    bias_half = of_rep(norm_bias, 0).reshape(1, -1)
    w_own = lax.dynamic_slice_in_dim(w_code, (dp * reps + rep) * block, block, 1)
    w_own = jnp.stack(
        [jnp.pad(w_own, ((0, 0), (q * block, LANES - (q + 1) * block))) for q in range(dims.groups)]
    )
    grads, stat = kernel_call(
        dims, middle_kernel,
        [((chips, dims.grad_rows, LANES), bf16), ((8, half), f32)],
        (place, recv, w_half, gain_half, bias_half, w_out_half, scale_row, shift_row), 1,
        "middle", 10**9,
    )
    share = lax.all_to_all(grads, "dp", split_axis=0, concat_axis=0, tiled=True)

    def whole(x):
        other = lax.ppermute(x, "rep", [(i, (i + 1) % reps) for i in range(reps)])
        halves = jnp.where(rep == 0, jnp.stack([x, other]), jnp.stack([other, x]))
        halves = halves.reshape(reps, 2, chips, block).transpose(1, 2, 0, 3)
        return halves.reshape(2, dims.hidden)

    total = recv[:, dims.send_rows - 8 :, :]
    row = dims.take + dims.stat_rows + 2 * dims.slots // LANES - (dims.send_rows - 8)
    total = total[:, row, 0].astype(jnp.float32).sum().astype(jnp.int32).reshape(1)
    moments = whole(stat[:2])
    (embedded,) = kernel_call(
        dims, embed_kernel, [((dims.slots, dims.width), bf16)],
        (
            counts, total, pre, moments[0:1], moments[1:2], norm_gain.reshape(1, -1),
            norm_bias.reshape(1, -1), w_out, out_bias.reshape(1, -1),
        ),
        2, "embed", 10**9,
    )
    packed = chips * dims.rows // dims.groups
    code, own_pre, live = kernel_call(
        dims, owner_kernel,
        [((dims.groups, packed, dims.codes), bf16), ((packed, LANES), f32), ((packed, LANES), f32)],
        (recv, w_own, scale_row, shift_row), 0, "owner", 4 * 10**9,
    )
    code_share, out_share, pair = kernel_call(
        dims, last_kernel,
        [((block, dims.codes), f32), ((block, dims.width), f32), ((8, half), f32)],
        (place, total, share, code, own_pre, live, stat, gain_half), 2, "last", 10**9,
    )
    grad_pair = whole(pair[:2])
    return embedded, code_share, out_share, grad_pair[0], grad_pair[1]


def solution(mesh):
    rows = P(AXES)

    def per_device(*arguments):
        ids, w_code, w_out = arguments[0], arguments[4], arguments[7]
        dims = Dims(mesh, ids.shape[0], w_code.shape[0], w_code.shape[1], w_out.shape[1])
        if dims.reps == 2 and dims.fits():
            return fast_device(dims, *arguments)
        return general_device(*arguments)

    return jax.shard_map(
        per_device,
        mesh=mesh,
        in_specs=(rows, rows, P(), P(), P(), P(), P(), P(), P(), P(AXES, None)),
        out_specs=(P(AXES, None), P(AXES, None), P(AXES, None), P(), P()),
        check_vma=False,
    )
```

```python
import functools
import math

import jax
import jax.numpy as jnp
from jax import lax
from jax.experimental import pallas as pl
from jax.experimental.pallas import tpu as pltpu
from jax.sharding import PartitionSpec as P

LANES = 128
modulus = 65521
epsilon = 1e-05
AXES = ("dp", "rep")


def hashed(ident, hash_scale, hash_shift):
    resid = ident % modulus
    bucket = (hash_scale[None, :] * resid[:, None] + hash_shift[None, :]) % modulus
    return (bucket.astype(jnp.float32) * (2.0 / (modulus - 1)) - 1.0).astype(jnp.bfloat16)


def mish_parts(gated):
    softer = jax.nn.softplus(gated)
    tangent = jnp.tanh(softer)
    return (gated * tangent, tangent + gated * (1.0 - tangent * tangent) * jax.nn.sigmoid(gated))


def exchange(blocks):
    return lax.all_to_all(blocks, AXES, split_axis=0, concat_axis=0, tiled=True)


def lane_rows(flat):
    pad = -flat.shape[-1] % (8 * LANES)
    flat = jnp.pad(flat, [(0, 0)] * (flat.ndim - 1) + [(0, pad)])
    return flat.reshape(flat.shape[:-1] + (-1, LANES))


def general_device(
    ids, counts, hash_scale, hash_shift, w_code, norm_gain, norm_bias, w_out, out_bias, cotangent
):
    devices = lax.axis_size("dp") * lax.axis_size("rep")
    me = lax.axis_index("dp") * lax.axis_size("rep") + lax.axis_index("rep")
    slots = ids.shape[0]
    codes, hidden = w_code.shape
    width = w_out.shape[1]
    share = hidden // devices
    keep = (jnp.arange(slots, dtype=jnp.int32) < counts[0])[:, None]

    preact = jnp.dot(
        hashed(ids, hash_scale, hash_shift), w_code, preferred_element_type=jnp.float32
    )
    masked = jnp.where(keep, preact, 0.0)
    row = lane_rows(
        jnp.concatenate(
            [
                masked.sum(0),
                (masked * masked).sum(0),
                ids.astype(jnp.float32),
                counts.astype(jnp.float32),
            ]
        )
    )
    table = exchange(jnp.broadcast_to(row, (devices,) + row.shape)).reshape(devices, -1)
    sums = table[:, : 2 * hidden].sum(0)
    all_ids = table[:, 2 * hidden : 2 * hidden + slots].astype(jnp.int32)
    all_counts = table[:, 2 * hidden + slots].astype(jnp.int32)
    total = all_counts.sum().astype(jnp.float32)
    mean = sums[:hidden] / total
    inv_std = lax.rsqrt(sums[hidden:] / total - mean * mean + epsilon)

    normed = (preact - mean) * inv_std
    act_full, slope = mish_parts(normed * norm_gain + norm_bias)
    act = act_full.astype(jnp.bfloat16)
    delta = jnp.where(keep, cotangent.astype(jnp.float32) * lax.rsqrt(total), 0.0).astype(
        jnp.bfloat16
    )
    dval = (
        lax.dot_general(delta, w_out, (((1,), (1,)), ((), ())), preferred_element_type=jnp.float32)
        * slope
    )
    grad_out = lax.dot_general(
        act, delta, (((0,), (0,)), ((), ())), preferred_element_type=jnp.float32
    )
    columns = exchange(dval.astype(jnp.bfloat16).T.reshape(devices, share, slots))
    pair = jnp.concatenate([(dval * normed).sum(0), dval.sum(0)])
    grads = exchange(
        lane_rows(
            jnp.concatenate(
                [
                    grad_out.reshape(devices, share * width),
                    jnp.broadcast_to(pair, (devices, 2 * hidden)),
                ],
                axis=1,
            )
        )
    )
    grads = grads.reshape(devices, -1)[:, : share * width + 2 * hidden].sum(0)
    out_share = grads[: share * width].reshape(share, width)
    grad_gain = grads[share * width : share * width + hidden]
    grad_bias = grads[share * width + hidden :]

    embedded = jnp.dot(act, w_out, preferred_element_type=jnp.float32) + out_bias
    embedded = jnp.where(keep, embedded, 0.0).astype(jnp.bfloat16)

    def own(vector):
        return lax.dynamic_slice_in_dim(vector, me * share, share, vector.ndim - 1)

    w_own = own(w_code)
    mean_own, inv_own = own(mean), own(inv_std)
    shift_own, tilt_own = own(grad_bias) / total, own(grad_gain) / total
    scale_own = own(norm_gain) * inv_own
    group = math.gcd(devices, max(1, 8192 // slots))

    def accumulate(index, grad_rows):
        start = index * group
        block_ids = lax.dynamic_slice_in_dim(all_ids, start, group, 0).reshape(-1)
        block_counts = lax.dynamic_slice_in_dim(all_counts, start, group, 0)
        block = lax.dynamic_slice_in_dim(columns, start, group, 0)
        code = hashed(block_ids, hash_scale, hash_shift)
        pre = lax.dot_general(
            w_own, code, (((0,), (1,)), ((), ())), preferred_element_type=jnp.float32
        )
        seen = (pre - mean_own[:, None]) * inv_own[:, None]
        dval_own = block.transpose(1, 0, 2).reshape(share, -1).astype(jnp.float32)
        dpre = scale_own[:, None] * (dval_own - shift_own[:, None] - seen * tilt_own[:, None])
        live = jnp.arange(slots, dtype=jnp.int32)[None, :] < block_counts[:, None]
        dpre = jnp.where(live.reshape(1, -1), dpre, 0.0).astype(jnp.bfloat16)
        return grad_rows + jnp.dot(dpre, code, preferred_element_type=jnp.float32)

    code_share = lax.fori_loop(
        0, devices // group, accumulate, jnp.zeros((share, codes), jnp.float32)
    )
    return embedded, code_share, out_share, grad_gain, grad_bias


def row_of(tiles):
    return jnp.concatenate(tiles, axis=1)


def place_block(tile, source, target, block):
    shift = ((target - source) * block) % LANES
    return pltpu.roll(tile, shift, 1) if shift else tile


def pick_blocks(x, chosen, block):
    per_tile = LANES // block
    lane = lax.broadcasted_iota(jnp.int32, (x.shape[0], LANES), 1) // block
    tiles = []
    for first in range(0, len(chosen), per_tile):
        tile = None
        for place, b in enumerate(chosen[first : first + per_tile]):
            start = b // per_tile * LANES
            piece = place_block(x[:, start : start + LANES], b % per_tile, place, block)
            tile = piece if tile is None else jnp.where(lane == place, piece, tile)
        tiles.append(tile)
    return tiles


def split_pair(x):
    high = x.astype(jnp.bfloat16).astype(jnp.float32)
    return high, (x - high).astype(jnp.bfloat16).astype(jnp.float32)


def codes_of(id_column, scale_row, shift_row):
    raw = scale_row * id_column + shift_row
    once = (raw - lax.shift_right_logical(raw, 16) * modulus).astype(jnp.float32)
    quotient = jnp.floor((once + 0.5) * (1.0 / modulus))
    bucket = once - quotient * float(modulus)
    return (bucket * (2.0 / (modulus - 1)) - 1.0).astype(jnp.bfloat16)


def mish_of(val):
    grown = jnp.exp(jnp.minimum(val, 20.0))
    n = grown * (grown + 2.0)
    inverse = 1.0 / (n + 2.0)
    t = n * inverse
    slope = t + val * (4.0 * grown * (1.0 + grown)) * (inverse * inverse)
    return val * t, slope


def dot_t(a, b):
    return lax.dot_general(a, b, (((1,), (1,)), ((), ())), preferred_element_type=jnp.float32)


def dot_rows(a, b):
    return lax.dot_general(a, b, (((0,), (0,)), ((), ())), preferred_element_type=jnp.float32)


def one_hot(condition):
    return jnp.where(condition, 1.0, 0.0).astype(jnp.bfloat16)


def id_bytes(ids_row):
    resid = lax.rem(ids_row, modulus)
    high = lax.shift_right_logical(resid, 8).astype(jnp.float32)
    low = lax.bitwise_and(resid, 255).astype(jnp.float32)
    return high, low, jnp.zeros((6, ids_row.shape[1]), jnp.float32)


def slot_codes(high, low, blank, scale_row, shift_row):
    slots = high.shape[1]
    same = one_hot(
        lax.broadcasted_iota(jnp.int32, (slots, slots), 0)
        == lax.broadcasted_iota(jnp.int32, (slots, slots), 1)
    )
    pieces = jnp.concatenate([high, low, blank], axis=0).astype(jnp.bfloat16)
    columns = dot_t(same, pieces)
    id_column = (columns[:, 0:1] * 256.0 + columns[:, 1:2]).astype(jnp.int32)
    return codes_of(id_column, scale_row, shift_row)


def first_kernel(
    dims, count_ref, ids_hbm, scale_hbm, shift_hbm, w_hbm, cot_hbm, send_ref,
    ids_ref, scale_ref, shift_ref, w_ref, cot_ref, sems,
):
    chips, reps, take, block = dims.chips, dims.reps, dims.take, dims.block
    slots = dims.slots
    copies = [
        pltpu.make_async_copy(source, target, sems.at[i])
        for i, (source, target) in enumerate(
            [
                (ids_hbm, ids_ref),
                (scale_hbm, scale_ref),
                (shift_hbm, shift_ref),
                (w_hbm, w_ref),
                (cot_hbm, cot_ref),
            ]
        )
    ]
    for copy in copies:
        copy.start()
    count = count_ref[0]
    r = lax.broadcasted_iota(jnp.int32, (slots, slots), 0)
    c = lax.broadcasted_iota(jnp.int32, (slots, slots), 1)
    order = one_hot(c == (r % take) * chips + r // take)
    for copy in copies[:3]:
        copy.wait()
    high, low, blank = id_bytes(ids_ref[...])
    codes = slot_codes(high, low, blank, scale_ref[...], shift_ref[...])
    live = lax.broadcasted_iota(jnp.int32, (1, slots), 1) < count
    marked = jnp.concatenate([jnp.where(live, high, 256.0), low, blank], axis=0)
    by_chip = dot_t(marked.astype(jnp.bfloat16), order)
    tail = [
        by_chip[i : i + 1, t * LANES : (t + 1) * LANES]
        for i in range(2)
        for t in range(slots // LANES)
    ]
    for copy in copies[3:]:
        copy.wait()
    pre = jnp.dot(codes, w_ref[...], preferred_element_type=jnp.float32)
    moved = jnp.dot(order, cot_ref[...], preferred_element_type=jnp.float32).astype(jnp.bfloat16)
    keep = lax.broadcasted_iota(jnp.int32, (slots, 1), 0) < count
    sums = jnp.where(keep, pre, 0.0).sum(0, keepdims=True)
    apart = jnp.where(keep, pre - sums / count.astype(jnp.float32), 0.0)
    spread = (apart * apart).sum(0, keepdims=True)
    stats = jnp.concatenate(split_pair(sums) + (spread,), axis=0)
    for rep in range(reps):
        tiles = pick_blocks(stats, [k * reps + rep for k in range(chips)], block)
        lower = jnp.concatenate(tiles + tail, axis=0).astype(jnp.bfloat16)
        for k in range(chips):
            send_ref[k * reps + rep, :take, :] = moved[k * take : (k + 1) * take, :]
            send_ref[k * reps + rep, take:, :] = lower


def id_rows(dims, recv):
    base = dims.take + dims.stat_rows
    parts = dims.slots // LANES
    rows = dims.devices * dims.take
    spread = one_hot(
        lax.broadcasted_iota(jnp.int32, (rows, dims.devices), 0) // dims.take
        == lax.broadcasted_iota(jnp.int32, (rows, dims.devices), 1)
    )
    own_j = (
        lax.broadcasted_iota(jnp.int32, (rows, dims.slots), 1) % dims.take
        == lax.broadcasted_iota(jnp.int32, (rows, dims.slots), 0) % dims.take
    )
    fold = one_hot(
        lax.broadcasted_iota(jnp.int32, (dims.chips, dims.slots), 1) // dims.take
        == lax.broadcasted_iota(jnp.int32, (dims.chips, dims.slots), 0)
    )
    flats = [
        row_of([recv[:, base + i * parts + t, :] for t in range(parts)]) for i in range(2)
    ]
    counts = jnp.where(flats[0] < 255.5, 1.0, 0.0).sum(1, keepdims=True)
    tables = []
    for flat in flats:
        wide = jnp.dot(spread, flat.astype(jnp.bfloat16), preferred_element_type=jnp.float32)
        tables.append(dot_t(fold, jnp.where(own_j, wide, 0.0).astype(jnp.bfloat16)))
    return counts, tables[0] * 256.0 + tables[1]


def packing(dims, counts, chip):
    lanes = dims.devices * dims.take
    d = lax.broadcasted_iota(jnp.int32, (dims.devices, lanes), 0)
    l = lax.broadcasted_iota(jnp.int32, (dims.devices, lanes), 1) // dims.take
    j = (lax.broadcasted_iota(jnp.int32, (1, lanes), 1) % dims.take).astype(jnp.float32)
    live = jnp.maximum(jnp.floor((counts - chip + (dims.chips - 1.0)) * (1.0 / dims.chips)), 0.0)
    before = jnp.where(d < l, live, 0.0).sum(0, keepdims=True)
    here = jnp.where(d == l, live, 0.0).sum(0, keepdims=True)
    target = jnp.where(j < here, before + j, -1.0).astype(jnp.int32)
    return target, live.sum(0, keepdims=True)


def middle_kernel(
    dims, place_ref, recv_ref, w_ref, gain_ref, bias_ref, w_out_ref, scale_ref, shift_ref, _,
    send_ref, stat_ref,
):
    take, block, rows = dims.take, dims.block, dims.rows
    half, groups = dims.half, dims.groups
    chip = place_ref[0]
    recv = recv_ref[:, take:, :].astype(jnp.float32)
    recv_all = jnp.concatenate([jnp.zeros((dims.devices, take, LANES), jnp.float32), recv], axis=1)
    counts, ids = id_rows(dims, recv_all)
    total = counts.sum(0, keepdims=True)
    target, _ = packing(dims, counts, chip.astype(jnp.float32))
    hit = lax.broadcasted_iota(jnp.int32, (rows, dims.devices * take), 0) == target
    own = lax.broadcasted_iota(jnp.int32, (dims.chips, 1), 0) == chip
    own_ids = jnp.where(own, ids, 0.0).sum(0, keepdims=True)
    id_column = jnp.where(hit, own_ids, 0.0).sum(1, keepdims=True).astype(jnp.int32)
    codes = codes_of(id_column, scale_ref[...], shift_ref[...])
    pre = jnp.dot(codes, w_ref[...], preferred_element_type=jnp.float32)
    cot = jnp.dot(
        one_hot(hit), recv_ref[:, :take, :].reshape(dims.devices * take, LANES),
        preferred_element_type=jnp.float32,
    )
    means, variances = [], []
    for t in range(half // LANES):
        r = 3 * t
        sums = recv[:, r, :] + recv[:, r + 1, :]
        mean = sums.sum(0, keepdims=True) / total
        off = sums / counts - mean
        means.append(mean)
        variances.append((recv[:, r + 2, :] + counts * (off * off)).sum(0, keepdims=True) / total)
    mean = row_of(means)
    inv_std = lax.rsqrt(row_of(variances) + epsilon)
    stat_ref[...] = jnp.concatenate(
        [mean, inv_std, jnp.zeros((6, half), jnp.float32) + total], axis=0
    )
    normed = (pre - mean) * inv_std
    act, slope = mish_of(normed * gain_ref[...] + bias_ref[...])
    delta = (cot * lax.rsqrt(total)).astype(jnp.bfloat16)
    dval = dot_t(delta, w_out_ref[...]) * slope
    grad_out = dot_rows(act.astype(jnp.bfloat16), delta).astype(jnp.bfloat16)
    pair = [(dval * normed).sum(0, keepdims=True), dval.sum(0, keepdims=True)]
    pair = jnp.concatenate(
        [x[:, t * LANES : (t + 1) * LANES] for x in pair for t in range(half // LANES)], axis=0
    ).astype(jnp.bfloat16)
    part = rows // groups
    lane = lax.broadcasted_iota(jnp.int32, (part, LANES), 1) // block
    for k in range(dims.chips):
        start = k // groups * LANES
        tile = None
        for q in range(groups):
            piece = dval[q * part : (q + 1) * part, start : start + LANES]
            piece = place_block(piece, k % groups, q, block)
            tile = piece if tile is None else jnp.where(lane == q, piece, tile)
        send_ref[k, :part, :] = tile.astype(jnp.bfloat16)
        send_ref[k, part : part + block, :] = grad_out[k * block : (k + 1) * block, :]
        send_ref[k, part + block :, :] = pair


def natural(dims, mine, other, rep):
    groups, reps, block = dims.groups, dims.reps, dims.block
    halves = [jnp.where(rep == 0, mine, other), jnp.where(rep == 0, other, mine)]
    lane = lax.broadcasted_iota(jnp.int32, (mine.shape[0], LANES), 1) // block
    tiles = []
    for first in range(0, dims.chips * reps, groups):
        tile = None
        for place in range(groups):
            k, p = (first + place) // reps, (first + place) % reps
            start = k // groups * LANES
            piece = place_block(halves[p][:, start : start + LANES], k % groups, place, block)
            tile = piece if tile is None else jnp.where(lane == place, piece, tile)
        tiles.append(tile)
    return row_of(tiles)


def embed_kernel(
    dims, count_ref, rep_ref, ids_ref, scale_ref, shift_ref, w_ref, mine_ref, other_ref, gain_ref,
    bias_ref, w_out_ref, out_bias_ref, out_ref, token_ref,
):
    codes = slot_codes(*id_bytes(ids_ref[...]), scale_ref[...], shift_ref[...])
    pre = jnp.dot(codes, w_ref[...], preferred_element_type=jnp.float32)
    moments = natural(dims, mine_ref[...], other_ref[...], rep_ref[0])
    normed = (pre - moments[0:1, :]) * moments[1:2, :]
    act, _ = mish_of(normed * gain_ref[...] + bias_ref[...])
    out = jnp.dot(act.astype(jnp.bfloat16), w_out_ref[...], preferred_element_type=jnp.float32)
    keep = lax.broadcasted_iota(jnp.int32, (dims.slots, 1), 0) < count_ref[0]
    out_ref[...] = jnp.where(keep, out + out_bias_ref[...], 0.0).astype(jnp.bfloat16)
    token_ref[...] = jnp.zeros((8, LANES), jnp.float32)


def spread_own(dims, x, chip):
    groups, block = dims.groups, dims.block
    lane = lax.broadcasted_iota(jnp.int32, (1, LANES), 1) // block
    own = jnp.zeros((1, LANES), jnp.float32)
    for t in range(dims.half // LANES):
        own = own + jnp.where(
            lane + t * groups == chip, x[:, t * LANES : (t + 1) * LANES], 0.0
        )
    out = own
    for i in range(1, groups):
        out = out + pltpu.roll(own, i * block, 1)
    return out


def owner_kernel(
    dims, place_ref, recv_ref, w_ref, scale_ref, shift_ref, stat_ref, _, fixed_ref, *code_refs
):
    counts, ids = id_rows(dims, recv_ref[...].astype(jnp.float32))
    part, block, groups = dims.rows // dims.groups, dims.block, dims.groups
    chip = place_ref[0]
    mean = spread_own(dims, stat_ref[0:1, :], chip)
    inv_std = spread_own(dims, stat_ref[1:2, :], chip)
    group = lax.broadcasted_iota(jnp.int32, (part, LANES), 1) // block
    row = lax.broadcasted_iota(jnp.int32, (part, LANES), 0)
    wide = lax.broadcasted_iota(jnp.int32, (dims.rows, dims.devices * dims.take), 0)
    pieces = [[] for _ in range(groups)]
    for s in range(dims.chips):
        target, live = packing(dims, counts, float(s))
        id_column = jnp.where(wide == target, ids[s : s + 1, :], 0.0).sum(1, keepdims=True)
        codes = codes_of(id_column.astype(jnp.int32), scale_ref[...], shift_ref[...])
        pre = jnp.dot(codes, w_ref[...], preferred_element_type=jnp.float32)
        for q in range(groups):
            code_refs[q][s * part : (s + 1) * part, :] = codes[q * part : (q + 1) * part, :]
            normed = (pre[q * part : (q + 1) * part, :] - mean) * inv_std
            piece = jnp.where(group == q, normed, jnp.where(group == (q + 1) % groups, 1.0, 0.0))
            piece = jnp.where((q * part + row).astype(jnp.float32) < live, piece, 0.0)
            pieces[q].append(piece)
    moved, plain = None, None
    for q in range(groups):
        term = dot_rows(
            jnp.concatenate(pieces[q], axis=0).astype(jnp.bfloat16), code_refs[q][...]
        )
        after = (q + 1) % groups
        own, ones = term[q * block : (q + 1) * block, :], term[after * block : (after + 1) * block, :]
        moved = own if moved is None else moved + own
        plain = ones if plain is None else plain + ones
    fixed_ref[:block, :] = moved
    fixed_ref[block:, :] = plain


def sums_kernel(dims, recv_ref, out_out_ref, pair_ref):
    part, block = dims.rows // dims.groups, dims.block
    pair = recv_ref[:, part + block :, :].astype(jnp.float32).sum(0)
    tiles = dims.half // LANES
    pair_ref[...] = jnp.concatenate(
        [row_of([pair[i * tiles + t : i * tiles + t + 1, :] for t in range(tiles)]) for i in range(2)]
        + [jnp.zeros((6, dims.half), jnp.float32)],
        axis=0,
    )
    out_out_ref[...] = recv_ref[:, part : part + block, :].astype(jnp.float32).sum(0)


def own_column(dims, x, chip):
    own = spread_own(dims, x, chip)
    spot = lax.broadcasted_iota(jnp.int32, (dims.block, LANES), 1)
    same = spot == lax.broadcasted_iota(jnp.int32, (dims.block, LANES), 0)
    return jnp.where(same, own, 0.0).sum(1, keepdims=True)


def last_kernel(
    dims, place_ref, recv_ref, fixed_ref, stat_ref, gain_ref, pair_ref, *refs
):
    part, block, groups = dims.rows // dims.groups, dims.block, dims.groups
    code_refs, code_out_ref, held, sems = list(refs[:groups]), refs[groups], refs[-2], refs[-1]
    copies = [
        pltpu.make_async_copy(code_refs[dims.near + i], held.at[i], sems.at[i])
        for i in range(groups - dims.near)
    ]
    for copy in copies:
        copy.start()
    chip = place_ref[0]
    total = stat_ref[2:3, :1]
    scale = own_column(dims, gain_ref[...] * stat_ref[1:2, :], chip)
    tilt = own_column(dims, pair_ref[0:1, :], chip) / total
    shift = own_column(dims, pair_ref[1:2, :], chip) / total
    dval = recv_ref[:, :part, :].reshape(dims.chips * part, LANES)
    out = -(shift * fixed_ref[block:, :] + tilt * fixed_ref[:block, :])
    for q in range(groups):
        if q >= dims.near:
            copies[q - dims.near].wait()
        code = code_refs[q][...] if q < dims.near else held[q - dims.near]
        out = out + dot_rows(dval, code)[q * block : (q + 1) * block, :]
    code_out_ref[...] = scale * out


def join_kernel(dims, rep_ref, mine_ref, other_ref, gain_ref, bias_ref):
    pair = natural(dims, mine_ref[...], other_ref[...], rep_ref[0])
    gain_ref[...] = pair[0:1, :]
    bias_ref[...] = pair[1:2, :]


class Dims:
    def __init__(self, mesh, slots, codes, hidden, width):
        self.chips, self.reps = mesh.shape["dp"], mesh.shape["rep"]
        self.devices = self.chips * self.reps
        self.slots, self.codes, self.hidden, self.width = slots, codes, hidden, width
        self.block = hidden // self.devices
        self.half = hidden // self.reps
        self.groups = LANES // max(1, self.block)
        self.near = self.groups // 2
        self.take = slots // self.chips
        bound = self.devices * slots // 4 // self.chips
        bound += self.devices * (self.chips - 1) // self.chips
        step = 8 * self.groups
        self.rows = min(-(-bound // step) * step, self.devices * self.take)
        self.stat_rows = 3 * self.half // LANES
        self.send_rows = self.take + self.stat_rows + 2 * slots // LANES
        self.grad_rows = self.rows // self.groups + self.block + 2 * self.half // LANES

    def fits(self):
        return (
            self.width == LANES
            and LANES % self.block == 0
            and self.block % 8 == 0
            and self.groups >= 2
            and self.take % 8 == 0
            and self.slots % LANES == 0
            and self.half % LANES == 0
            and self.codes % LANES == 0
            and self.chips <= LANES
            and self.slots <= 256
            and self.rows % (8 * self.groups) == 0
            and self.chips * self.rows * self.codes <= (1 << 22)
        )


def kernel_call(dims, body, outs, arguments, scalars, name, flops, hbm=(), scratch=(), vmem=16):
    specs = [pl.BlockSpec(memory_space=pltpu.SMEM)] * scalars
    for i in range(scalars, len(arguments)):
        specs.append(pl.BlockSpec(memory_space=pltpu.HBM if i in hbm else pltpu.VMEM))
    return pl.pallas_call(
        functools.partial(body, dims),
        out_shape=[jax.ShapeDtypeStruct(shape, kind) for shape, kind in outs],
        in_specs=specs,
        out_specs=[pl.BlockSpec(memory_space=pltpu.VMEM)] * len(outs),
        scratch_shapes=list(scratch),
        compiler_params=pltpu.CompilerParams(vmem_limit_bytes=vmem << 20),
        cost_estimate=pl.CostEstimate(flops=flops, bytes_accessed=1 << 20, transcendentals=0),
        name=name,
    )(*arguments)


def fast_device(
    dims, ids, counts, hash_scale, hash_shift, w_code, norm_gain, norm_bias, w_out, out_bias,
    cotangent,
):
    chips, reps, block, half = dims.chips, dims.reps, dims.block, dims.half
    dp, rep = lax.axis_index("dp"), lax.axis_index("rep")
    f32, bf16 = jnp.float32, jnp.bfloat16
    ids = ids.reshape(1, -1)
    scale_row, shift_row = hash_scale.reshape(1, -1), hash_shift.reshape(1, -1)
    loaded = (ids, scale_row, shift_row, w_code, cotangent)
    (send,) = kernel_call(
        dims, first_kernel,
        [((dims.devices, dims.send_rows, LANES), bf16)],
        (counts,) + loaded, 1, "first", 10**9, hbm=(1, 2, 3, 4, 5),
        scratch=[pltpu.VMEM(x.shape, x.dtype) for x in loaded]
        + [pltpu.SemaphoreType.DMA((len(loaded),))], vmem=60,
    )
    recv = exchange(send)

    def of_rep(x, axis):
        shape = x.shape[:axis] + (chips, reps, block) + x.shape[axis + 1 :]
        x = lax.dynamic_index_in_dim(x.reshape(shape), rep, axis + 1, keepdims=False)
        return x.reshape(x.shape[:axis] + (half,) + x.shape[axis + 2 :])

    place, side = dp.reshape(1).astype(jnp.int32), rep.reshape(1).astype(jnp.int32)
    w_half, w_out_half = of_rep(w_code, 1), of_rep(w_out, 0)
    gain_half = of_rep(norm_gain, 0).reshape(1, -1)
    bias_half = of_rep(norm_bias, 0).reshape(1, -1)
    w_own = lax.dynamic_slice_in_dim(w_code, (dp * reps + rep) * block, block, 1)
    w_own = jnp.concatenate([w_own] * dims.groups, axis=1)
    grads, stat = kernel_call(
        dims, middle_kernel,
        [((chips, dims.grad_rows, LANES), bf16), ((8, half), f32)],
        (place, recv, w_half, gain_half, bias_half, w_out_half, scale_row, shift_row, w_own), 1,
        "middle", 10**9,
    )
    share = lax.all_to_all(grads, "dp", split_axis=0, concat_axis=0, tiled=True)

    def partner(x):
        return lax.ppermute(x, "rep", [(i, (i + 1) % reps) for i in range(reps)])

    packed = chips * dims.rows // dims.groups
    embedded, token = kernel_call(
        dims, embed_kernel, [((dims.slots, dims.width), bf16), ((8, LANES), f32)],
        (
            counts, side, ids, scale_row, shift_row, w_code, stat, partner(stat), norm_gain.reshape(1, -1),
            norm_bias.reshape(1, -1), w_out, out_bias.reshape(1, -1),
        ),
        2, "embed", 10**9,
    )
    fixed, *code = kernel_call(
        dims, owner_kernel,
        [((2 * block, dims.codes), f32)] + [((packed, dims.codes), bf16)] * dims.groups,
        (place, recv, w_own, scale_row, shift_row, stat, token), 1, "owner", 4 * 10**9,
    )
    out_share, pair = kernel_call(
        dims, sums_kernel, [((block, dims.width), f32), ((8, half), f32)],
        (share,), 0, "sums", 10**8,
    )
    other = partner(pair)
    (code_share,) = kernel_call(
        dims, last_kernel, [((block, dims.codes), f32)],
        (
            place, share, fixed, stat, gain_half, pair, *code[: dims.near],
            *[pltpu.with_memory_space_constraint(x, pltpu.HBM) for x in code[dims.near :]],
        ),
        1, "last", 10**9, hbm=range(6 + dims.near, 6 + dims.groups),
        scratch=[
            pltpu.VMEM((dims.groups - dims.near, packed, dims.codes), bf16),
            pltpu.SemaphoreType.DMA((dims.groups - dims.near,)),
        ],
    )
    gain, bias = kernel_call(
        dims, join_kernel, [((1, dims.hidden), f32)] * 2, (side, pair, other), 1, "join", 10**6
    )
    return embedded, code_share, out_share, gain.reshape(-1), bias.reshape(-1)


def solution(mesh):
    rows = P(AXES)

    def per_device(*arguments):
        ids, w_code, w_out = arguments[0], arguments[4], arguments[7]
        dims = Dims(mesh, ids.shape[0], w_code.shape[0], w_code.shape[1], w_out.shape[1])
        if dims.reps == 2 and dims.fits():
            return fast_device(dims, *arguments)
        return general_device(*arguments)

    return jax.shard_map(
        per_device,
        mesh=mesh,
        in_specs=(rows, rows, P(), P(), P(), P(), P(), P(), P(), P(AXES, None)),
        out_specs=(P(AXES, None), P(AXES, None), P(AXES, None), P(), P()),
        check_vma=False,
    )
```

```python
import functools
import math

import jax
import jax.numpy as jnp
from jax import lax
from jax.experimental import pallas as pl
from jax.experimental.pallas import tpu as pltpu
from jax.sharding import PartitionSpec as P

LANES = 128
PARTS = 4
modulus = 65521
epsilon = 1e-05
AXES = ("dp", "rep")


def hashed(ident, hash_scale, hash_shift):
    resid = ident % modulus
    bucket = (hash_scale[None, :] * resid[:, None] + hash_shift[None, :]) % modulus
    return (bucket.astype(jnp.float32) * (2.0 / (modulus - 1)) - 1.0).astype(jnp.bfloat16)


def mish_parts(gated):
    softer = jax.nn.softplus(gated)
    tangent = jnp.tanh(softer)
    return (gated * tangent, tangent + gated * (1.0 - tangent * tangent) * jax.nn.sigmoid(gated))


def exchange(blocks):
    return lax.all_to_all(blocks, AXES, split_axis=0, concat_axis=0, tiled=True)


def lane_rows(flat):
    pad = -flat.shape[-1] % (8 * LANES)
    flat = jnp.pad(flat, [(0, 0)] * (flat.ndim - 1) + [(0, pad)])
    return flat.reshape(flat.shape[:-1] + (-1, LANES))


def general_device(
    ids, counts, hash_scale, hash_shift, w_code, norm_gain, norm_bias, w_out, out_bias, cotangent
):
    devices = lax.axis_size("dp") * lax.axis_size("rep")
    me = lax.axis_index("dp") * lax.axis_size("rep") + lax.axis_index("rep")
    slots = ids.shape[0]
    codes, hidden = w_code.shape
    width = w_out.shape[1]
    share = hidden // devices
    keep = (jnp.arange(slots, dtype=jnp.int32) < counts[0])[:, None]

    preact = jnp.dot(
        hashed(ids, hash_scale, hash_shift), w_code, preferred_element_type=jnp.float32
    )
    masked = jnp.where(keep, preact, 0.0)
    row = lane_rows(
        jnp.concatenate(
            [
                masked.sum(0),
                (masked * masked).sum(0),
                ids.astype(jnp.float32),
                counts.astype(jnp.float32),
            ]
        )
    )
    table = exchange(jnp.broadcast_to(row, (devices,) + row.shape)).reshape(devices, -1)
    sums = table[:, : 2 * hidden].sum(0)
    all_ids = table[:, 2 * hidden : 2 * hidden + slots].astype(jnp.int32)
    all_counts = table[:, 2 * hidden + slots].astype(jnp.int32)
    total = all_counts.sum().astype(jnp.float32)
    mean = sums[:hidden] / total
    inv_std = lax.rsqrt(sums[hidden:] / total - mean * mean + epsilon)

    normed = (preact - mean) * inv_std
    act_full, slope = mish_parts(normed * norm_gain + norm_bias)
    act = act_full.astype(jnp.bfloat16)
    delta = jnp.where(keep, cotangent.astype(jnp.float32) * lax.rsqrt(total), 0.0).astype(
        jnp.bfloat16
    )
    dval = (
        lax.dot_general(delta, w_out, (((1,), (1,)), ((), ())), preferred_element_type=jnp.float32)
        * slope
    )
    grad_out = lax.dot_general(
        act, delta, (((0,), (0,)), ((), ())), preferred_element_type=jnp.float32
    )
    columns = exchange(dval.astype(jnp.bfloat16).T.reshape(devices, share, slots))
    pair = jnp.concatenate([(dval * normed).sum(0), dval.sum(0)])
    grads = exchange(
        lane_rows(
            jnp.concatenate(
                [
                    grad_out.reshape(devices, share * width),
                    jnp.broadcast_to(pair, (devices, 2 * hidden)),
                ],
                axis=1,
            )
        )
    )
    grads = grads.reshape(devices, -1)[:, : share * width + 2 * hidden].sum(0)
    out_share = grads[: share * width].reshape(share, width)
    grad_gain = grads[share * width : share * width + hidden]
    grad_bias = grads[share * width + hidden :]

    embedded = jnp.dot(act, w_out, preferred_element_type=jnp.float32) + out_bias
    embedded = jnp.where(keep, embedded, 0.0).astype(jnp.bfloat16)

    def own(vector):
        return lax.dynamic_slice_in_dim(vector, me * share, share, vector.ndim - 1)

    w_own = own(w_code)
    mean_own, inv_own = own(mean), own(inv_std)
    shift_own, tilt_own = own(grad_bias) / total, own(grad_gain) / total
    scale_own = own(norm_gain) * inv_own
    group = math.gcd(devices, max(1, 8192 // slots))

    def accumulate(index, grad_rows):
        start = index * group
        block_ids = lax.dynamic_slice_in_dim(all_ids, start, group, 0).reshape(-1)
        block_counts = lax.dynamic_slice_in_dim(all_counts, start, group, 0)
        block = lax.dynamic_slice_in_dim(columns, start, group, 0)
        code = hashed(block_ids, hash_scale, hash_shift)
        pre = lax.dot_general(
            w_own, code, (((0,), (1,)), ((), ())), preferred_element_type=jnp.float32
        )
        seen = (pre - mean_own[:, None]) * inv_own[:, None]
        dval_own = block.transpose(1, 0, 2).reshape(share, -1).astype(jnp.float32)
        dpre = scale_own[:, None] * (dval_own - shift_own[:, None] - seen * tilt_own[:, None])
        live = jnp.arange(slots, dtype=jnp.int32)[None, :] < block_counts[:, None]
        dpre = jnp.where(live.reshape(1, -1), dpre, 0.0).astype(jnp.bfloat16)
        return grad_rows + jnp.dot(dpre, code, preferred_element_type=jnp.float32)

    code_share = lax.fori_loop(
        0, devices // group, accumulate, jnp.zeros((share, codes), jnp.float32)
    )
    return embedded, code_share, out_share, grad_gain, grad_bias


def row_of(tiles):
    return jnp.concatenate(tiles, axis=1)


def place_block(tile, source, target, block):
    shift = ((target - source) * block) % LANES
    return pltpu.roll(tile, shift, 1) if shift else tile


def pick_blocks(x, chosen, block):
    per_tile = LANES // block
    lane = lax.broadcasted_iota(jnp.int32, (x.shape[0], LANES), 1) // block
    tiles = []
    for first in range(0, len(chosen), per_tile):
        tile = None
        for place, b in enumerate(chosen[first : first + per_tile]):
            start = b // per_tile * LANES
            piece = place_block(x[:, start : start + LANES], b % per_tile, place, block)
            tile = piece if tile is None else jnp.where(lane == place, piece, tile)
        tiles.append(tile)
    return tiles


def split_pair(x):
    high = x.astype(jnp.bfloat16).astype(jnp.float32)
    return high, (x - high).astype(jnp.bfloat16).astype(jnp.float32)


def codes_of(id_column, scale_row, shift_row):
    raw = scale_row * id_column + shift_row
    once = (raw - lax.shift_right_logical(raw, 16) * modulus).astype(jnp.float32)
    quotient = jnp.floor((once + 0.5) * (1.0 / modulus))
    bucket = once - quotient * float(modulus)
    return (bucket * (2.0 / (modulus - 1)) - 1.0).astype(jnp.bfloat16)


def mish_of(val):
    grown = jnp.exp(jnp.minimum(val, 20.0))
    n = grown * (grown + 2.0)
    inverse = 1.0 / (n + 2.0)
    t = n * inverse
    slope = t + val * (4.0 * grown * (1.0 + grown)) * (inverse * inverse)
    return val * t, slope


def dot_t(a, b):
    return lax.dot_general(a, b, (((1,), (1,)), ((), ())), preferred_element_type=jnp.float32)


def dot_rows(a, b):
    return lax.dot_general(a, b, (((0,), (0,)), ((), ())), preferred_element_type=jnp.float32)


def one_hot(condition):
    return jnp.where(condition, 1.0, 0.0).astype(jnp.bfloat16)


def id_bytes(ids_row):
    resid = lax.rem(ids_row, modulus)
    high = lax.shift_right_logical(resid, 8).astype(jnp.float32)
    low = lax.bitwise_and(resid, 255).astype(jnp.float32)
    return high, low, jnp.zeros((6, ids_row.shape[1]), jnp.float32)


def slot_codes(high, low, blank, scale_row, shift_row):
    slots = high.shape[1]
    same = one_hot(
        lax.broadcasted_iota(jnp.int32, (slots, slots), 0)
        == lax.broadcasted_iota(jnp.int32, (slots, slots), 1)
    )
    pieces = jnp.concatenate([high, low, blank], axis=0).astype(jnp.bfloat16)
    columns = dot_t(same, pieces)
    id_column = (columns[:, 0:1] * 256.0 + columns[:, 1:2]).astype(jnp.int32)
    return codes_of(id_column, scale_row, shift_row)


def first_kernel(
    dims, count_ref, ids_hbm, scale_hbm, shift_hbm, w_hbm, cot_hbm, send_ref,
    ids_ref, scale_ref, shift_ref, w_ref, cot_ref, sems,
):
    chips, reps, take, block = dims.chips, dims.reps, dims.take, dims.block
    slots = dims.slots
    copies = [
        pltpu.make_async_copy(source, target, sems.at[i])
        for i, (source, target) in enumerate(
            [
                (ids_hbm, ids_ref),
                (scale_hbm, scale_ref),
                (shift_hbm, shift_ref),
                (w_hbm, w_ref),
                (cot_hbm, cot_ref),
            ]
        )
    ]
    for copy in copies:
        copy.start()
    count = count_ref[0]
    r = lax.broadcasted_iota(jnp.int32, (slots, slots), 0)
    c = lax.broadcasted_iota(jnp.int32, (slots, slots), 1)
    order = one_hot(c == (r % take) * chips + r // take)
    for copy in copies[:3]:
        copy.wait()
    high, low, blank = id_bytes(ids_ref[...])
    codes = slot_codes(high, low, blank, scale_ref[...], shift_ref[...])
    live = lax.broadcasted_iota(jnp.int32, (1, slots), 1) < count
    marked = jnp.concatenate([jnp.where(live, high, 256.0), low, blank], axis=0)
    by_chip = dot_t(marked.astype(jnp.bfloat16), order)
    tail = [
        by_chip[i : i + 1, t * LANES : (t + 1) * LANES]
        for i in range(2)
        for t in range(slots // LANES)
    ]
    for copy in copies[3:]:
        copy.wait()
    pre = jnp.dot(codes, w_ref[...], preferred_element_type=jnp.float32)
    moved = jnp.dot(order, cot_ref[...], preferred_element_type=jnp.float32).astype(jnp.bfloat16)
    keep = lax.broadcasted_iota(jnp.int32, (slots, 1), 0) < count
    sums = jnp.where(keep, pre, 0.0).sum(0, keepdims=True)
    apart = jnp.where(keep, pre - sums / count.astype(jnp.float32), 0.0)
    spread = (apart * apart).sum(0, keepdims=True)
    stats = jnp.concatenate(split_pair(sums) + (spread,), axis=0)
    for rep in range(reps):
        tiles = pick_blocks(stats, [k * reps + rep for k in range(chips)], block)
        lower = jnp.concatenate(tiles + tail, axis=0).astype(jnp.bfloat16)
        for k in range(chips):
            send_ref[k * reps + rep, :take, :] = moved[k * take : (k + 1) * take, :]
            send_ref[k * reps + rep, take:, :] = lower


def id_rows(dims, recv):
    base = dims.take + dims.stat_rows
    parts = dims.slots // LANES
    rows = dims.devices * dims.take
    spread = one_hot(
        lax.broadcasted_iota(jnp.int32, (rows, dims.devices), 0) // dims.take
        == lax.broadcasted_iota(jnp.int32, (rows, dims.devices), 1)
    )
    own_j = (
        lax.broadcasted_iota(jnp.int32, (rows, dims.slots), 1) % dims.take
        == lax.broadcasted_iota(jnp.int32, (rows, dims.slots), 0) % dims.take
    )
    fold = one_hot(
        lax.broadcasted_iota(jnp.int32, (dims.chips, dims.slots), 1) // dims.take
        == lax.broadcasted_iota(jnp.int32, (dims.chips, dims.slots), 0)
    )
    flats = [
        row_of([recv[:, base + i * parts + t, :] for t in range(parts)]) for i in range(2)
    ]
    counts = jnp.where(flats[0] < 255.5, 1.0, 0.0).sum(1, keepdims=True)
    tables = []
    for flat in flats:
        wide = jnp.dot(spread, flat.astype(jnp.bfloat16), preferred_element_type=jnp.float32)
        tables.append(dot_t(fold, jnp.where(own_j, wide, 0.0).astype(jnp.bfloat16)))
    return counts, tables[0] * 256.0 + tables[1]


def packing(dims, counts, chip):
    lanes = dims.devices * dims.take
    d = lax.broadcasted_iota(jnp.int32, (dims.devices, lanes), 0)
    l = lax.broadcasted_iota(jnp.int32, (dims.devices, lanes), 1) // dims.take
    j = (lax.broadcasted_iota(jnp.int32, (1, lanes), 1) % dims.take).astype(jnp.float32)
    live = jnp.maximum(jnp.floor((counts - chip + (dims.chips - 1.0)) * (1.0 / dims.chips)), 0.0)
    before = jnp.where(d < l, live, 0.0).sum(0, keepdims=True)
    here = jnp.where(d == l, live, 0.0).sum(0, keepdims=True)
    target = jnp.where(j < here, before + j, -1.0).astype(jnp.int32)
    return target, live.sum(0, keepdims=True)


def middle_kernel(
    dims, place_ref, recv_ref, w_ref, gain_ref, bias_ref, w_out_ref, scale_ref, shift_ref, _,
    send_ref, stat_ref, ids_ref, counts_ref,
):
    take, block, rows = dims.take, dims.block, dims.rows
    half, groups = dims.half, dims.groups
    chip = place_ref[0]
    recv = recv_ref[:, take:, :].astype(jnp.float32)
    recv_all = jnp.concatenate([jnp.zeros((dims.devices, take, LANES), jnp.float32), recv], axis=1)
    counts, ids = id_rows(dims, recv_all)
    ids_ref[...] = ids
    counts_ref[...] = jnp.zeros((dims.devices, LANES), jnp.float32) + counts
    total = counts.sum(0, keepdims=True)
    target, _ = packing(dims, counts, chip.astype(jnp.float32))
    hit = lax.broadcasted_iota(jnp.int32, (rows, dims.devices * take), 0) == target
    own = lax.broadcasted_iota(jnp.int32, (dims.chips, 1), 0) == chip
    own_ids = jnp.where(own, ids, 0.0).sum(0, keepdims=True)
    id_column = jnp.where(hit, own_ids, 0.0).sum(1, keepdims=True).astype(jnp.int32)
    codes = codes_of(id_column, scale_ref[...], shift_ref[...])
    pre = jnp.dot(codes, w_ref[...], preferred_element_type=jnp.float32)
    cot = jnp.dot(
        one_hot(hit), recv_ref[:, :take, :].reshape(dims.devices * take, LANES),
        preferred_element_type=jnp.float32,
    )
    means, variances = [], []
    for t in range(half // LANES):
        r = 3 * t
        sums = recv[:, r, :] + recv[:, r + 1, :]
        mean = sums.sum(0, keepdims=True) / total
        off = sums / counts - mean
        means.append(mean)
        variances.append((recv[:, r + 2, :] + counts * (off * off)).sum(0, keepdims=True) / total)
    mean = row_of(means)
    inv_std = lax.rsqrt(row_of(variances) + epsilon)
    stat_ref[...] = jnp.concatenate(
        [mean, inv_std, jnp.zeros((6, half), jnp.float32) + total], axis=0
    )
    normed = (pre - mean) * inv_std
    act, slope = mish_of(normed * gain_ref[...] + bias_ref[...])
    delta = (cot * lax.rsqrt(total)).astype(jnp.bfloat16)
    dval = dot_t(delta, w_out_ref[...]) * slope
    grad_out = dot_rows(act.astype(jnp.bfloat16), delta).astype(jnp.bfloat16)
    pair = [(dval * normed).sum(0, keepdims=True), dval.sum(0, keepdims=True)]
    pair = jnp.concatenate(
        [x[:, t * LANES : (t + 1) * LANES] for x in pair for t in range(half // LANES)], axis=0
    ).astype(jnp.bfloat16)
    part = rows // groups
    lane = lax.broadcasted_iota(jnp.int32, (part, LANES), 1) // block
    for k in range(dims.chips):
        start = k // groups * LANES
        tile = None
        for q in range(groups):
            piece = dval[q * part : (q + 1) * part, start : start + LANES]
            piece = place_block(piece, k % groups, q, block)
            tile = piece if tile is None else jnp.where(lane == q, piece, tile)
        send_ref[k, :part, :] = tile.astype(jnp.bfloat16)
        send_ref[k, part : part + block, :] = grad_out[k * block : (k + 1) * block, :]
        send_ref[k, part + block :, :] = pair


def natural(dims, mine, other, rep):
    groups, reps, block = dims.groups, dims.reps, dims.block
    halves = [jnp.where(rep == 0, mine, other), jnp.where(rep == 0, other, mine)]
    lane = lax.broadcasted_iota(jnp.int32, (mine.shape[0], LANES), 1) // block
    tiles = []
    for first in range(0, dims.chips * reps, groups):
        tile = None
        for place in range(groups):
            k, p = (first + place) // reps, (first + place) % reps
            start = k // groups * LANES
            piece = place_block(halves[p][:, start : start + LANES], k % groups, place, block)
            tile = piece if tile is None else jnp.where(lane == place, piece, tile)
        tiles.append(tile)
    return row_of(tiles)


def embed_kernel(
    dims, count_ref, rep_ref, ids_ref, scale_ref, shift_ref, w_hbm, mine_ref, other_ref, gain_ref,
    bias_ref, w_out_hbm, out_bias_ref, out_ref, token_ref, w_ref, w_out_ref, sems,
):
    cut = dims.codes // 2
    copies = [
        pltpu.make_async_copy(
            w_hbm.at[pl.ds(i * cut, cut)], w_ref.at[pl.ds(i * cut, cut)], sems.at[i]
        )
        for i in range(2)
    ]
    copies.append(pltpu.make_async_copy(w_out_hbm, w_out_ref, sems.at[2]))
    for copy in copies:
        copy.start()
    codes = slot_codes(*id_bytes(ids_ref[...]), scale_ref[...], shift_ref[...])
    copies[0].wait()
    pre = jnp.dot(codes[:, :cut], w_ref[:cut, :], preferred_element_type=jnp.float32)
    copies[1].wait()
    pre = pre + jnp.dot(codes[:, cut:], w_ref[cut:, :], preferred_element_type=jnp.float32)
    copies[2].wait()
    moments = natural(dims, mine_ref[...], other_ref[...], rep_ref[0])
    normed = (pre - moments[0:1, :]) * moments[1:2, :]
    act, _ = mish_of(normed * gain_ref[...] + bias_ref[...])
    out = jnp.dot(act.astype(jnp.bfloat16), w_out_ref[...], preferred_element_type=jnp.float32)
    keep = lax.broadcasted_iota(jnp.int32, (dims.slots, 1), 0) < count_ref[0]
    out_ref[...] = jnp.where(keep, out + out_bias_ref[...], 0.0).astype(jnp.bfloat16)
    token_ref[...] = jnp.zeros((8, LANES), jnp.float32)


def spread_own(dims, x, chip):
    groups, block = dims.groups, dims.block
    lane = lax.broadcasted_iota(jnp.int32, (1, LANES), 1) // block
    own = jnp.zeros((1, LANES), jnp.float32)
    for t in range(dims.half // LANES):
        own = own + jnp.where(
            lane + t * groups == chip, x[:, t * LANES : (t + 1) * LANES], 0.0
        )
    out = own
    for i in range(1, groups):
        out = out + pltpu.roll(own, i * block, 1)
    return out


def codes_of_group(dims, code_refs, q):
    return jnp.concatenate(
        [ref[...] for ref in code_refs[q * dims.parts : (q + 1) * dims.parts]], axis=0
    )


def owner_kernel(
    dims, place_ref, ids_ref, counts_ref, w_ref, scale_ref, shift_ref, stat_ref, _, fixed_ref,
    *code_refs,
):
    counts = counts_ref[:, 0:1]
    part, block, groups = dims.rows // dims.groups, dims.block, dims.groups
    chip = place_ref[0]
    mean = spread_own(dims, stat_ref[0:1, :], chip)
    inv_std = spread_own(dims, stat_ref[1:2, :], chip)
    group = lax.broadcasted_iota(jnp.int32, (part, LANES), 1) // block
    row = lax.broadcasted_iota(jnp.int32, (part, LANES), 0)
    wide = lax.broadcasted_iota(jnp.int32, (dims.rows, dims.devices * dims.take), 0)
    pieces = [[] for _ in range(groups)]
    for s in range(dims.chips):
        target, live = packing(dims, counts, float(s))
        id_column = jnp.where(wide == target, ids_ref[s : s + 1, :], 0.0).sum(1, keepdims=True)
        codes = codes_of(id_column.astype(jnp.int32), scale_ref[...], shift_ref[...])
        pre = jnp.dot(codes, w_ref[...], preferred_element_type=jnp.float32)
        for q in range(groups):
            start = s * part
            code_refs[q * dims.parts + start // dims.piece][
                start % dims.piece : start % dims.piece + part, :
            ] = codes[q * part : (q + 1) * part, :]
            normed = (pre[q * part : (q + 1) * part, :] - mean) * inv_std
            piece = jnp.where(group == q, normed, jnp.where(group == (q + 1) % groups, 1.0, 0.0))
            piece = jnp.where((q * part + row).astype(jnp.float32) < live, piece, 0.0)
            pieces[q].append(piece)
    moved, plain = None, None
    for q in range(groups):
        term = dot_rows(
            jnp.concatenate(pieces[q], axis=0).astype(jnp.bfloat16), codes_of_group(dims, code_refs, q)
        )
        after = (q + 1) % groups
        own, ones = term[q * block : (q + 1) * block, :], term[after * block : (after + 1) * block, :]
        moved = own if moved is None else moved + own
        plain = ones if plain is None else plain + ones
    fixed_ref[:block, :] = moved
    fixed_ref[block:, :] = plain[:8, :]


def pair_sums(dims, rows):
    pair = rows.astype(jnp.float32).sum(0)
    tiles = dims.half // LANES
    return [
        row_of([pair[i * tiles + t : i * tiles + t + 1, :] for t in range(tiles)]) for i in range(2)
    ]


def own_column(dims, x, chip):
    own = spread_own(dims, x, chip)
    spot = lax.broadcasted_iota(jnp.int32, (dims.block, LANES), 1)
    same = spot == lax.broadcasted_iota(jnp.int32, (dims.block, LANES), 0)
    return jnp.where(same, own, 0.0).sum(1, keepdims=True)


def last_kernel(
    dims, place_ref, recv_ref, fixed_ref, stat_ref, gain_ref, *refs
):
    part, block, groups = dims.rows // dims.groups, dims.block, dims.groups
    code_refs, (code_out_ref, out_out_ref) = refs[:-2], refs[-2:]
    chip = place_ref[0]
    total = stat_ref[2:3, :1]
    scale = own_column(dims, gain_ref[...] * stat_ref[1:2, :], chip)
    gain, bias = pair_sums(dims, recv_ref[:, part + block :, :])
    tilt = own_column(dims, gain, chip) / total
    shift = own_column(dims, bias, chip) / total
    out_out_ref[...] = recv_ref[:, part : part + block, :].astype(jnp.float32).sum(0)
    dval = recv_ref[:, :part, :].reshape(dims.chips * part, LANES)
    out = -(shift * fixed_ref[block : block + 1, :] + tilt * fixed_ref[:block, :])
    for q in range(groups):
        out = out + dot_rows(dval, codes_of_group(dims, code_refs, q))[q * block : (q + 1) * block, :]
    code_out_ref[...] = scale * out


def join_kernel(dims, rep_ref, mine_ref, other_ref, gain_ref, bias_ref):
    blank = jnp.zeros((6, dims.half), jnp.float32)
    mine, other = (
        jnp.concatenate(pair_sums(dims, ref[...]) + [blank], axis=0) for ref in (mine_ref, other_ref)
    )
    pair = natural(dims, mine, other, rep_ref[0])
    gain_ref[...] = pair[0:1, :]
    bias_ref[...] = pair[1:2, :]


class Dims:
    def __init__(self, mesh, slots, codes, hidden, width):
        self.chips, self.reps = mesh.shape["dp"], mesh.shape["rep"]
        self.devices = self.chips * self.reps
        self.slots, self.codes, self.hidden, self.width = slots, codes, hidden, width
        self.block = hidden // self.devices
        self.half = hidden // self.reps
        self.groups = LANES // max(1, self.block)
        self.take = slots // self.chips
        self.parts = PARTS
        bound = self.devices * slots // 4 // self.chips
        bound += self.devices * (self.chips - 1) // self.chips
        step = 8 * self.groups
        self.rows = min(-(-bound // step) * step, self.devices * self.take)
        self.piece = self.chips * self.rows // self.groups // self.parts
        self.stat_rows = 3 * self.half // LANES
        self.send_rows = self.take + self.stat_rows + 2 * slots // LANES
        self.grad_rows = self.rows // self.groups + self.block + 2 * self.half // LANES

    def fits(self):
        return (
            self.width == LANES
            and LANES % self.block == 0
            and self.block % 8 == 0
            and self.chips % self.parts == 0
            and self.take % 8 == 0
            and self.slots % LANES == 0
            and self.half % LANES == 0
            and self.codes % LANES == 0
            and self.chips <= LANES
            and self.slots <= 256
            and self.rows % (8 * self.groups) == 0
            and self.chips * self.rows * self.codes <= (1 << 22)
        )


def kernel_call(dims, body, outs, arguments, scalars, name, flops, hbm=(), scratch=(), vmem=16):
    specs = [pl.BlockSpec(memory_space=pltpu.SMEM)] * scalars
    for i in range(scalars, len(arguments)):
        specs.append(pl.BlockSpec(memory_space=pltpu.HBM if i in hbm else pltpu.VMEM))
    return pl.pallas_call(
        functools.partial(body, dims),
        out_shape=[jax.ShapeDtypeStruct(shape, kind) for shape, kind in outs],
        in_specs=specs,
        out_specs=[pl.BlockSpec(memory_space=pltpu.VMEM)] * len(outs),
        scratch_shapes=list(scratch),
        compiler_params=pltpu.CompilerParams(vmem_limit_bytes=vmem << 20),
        cost_estimate=pl.CostEstimate(flops=flops, bytes_accessed=1 << 20, transcendentals=0),
        name=name,
    )(*arguments)


def fast_device(
    dims, ids, counts, hash_scale, hash_shift, w_code, norm_gain, norm_bias, w_out, out_bias,
    cotangent,
):
    chips, reps, block, half = dims.chips, dims.reps, dims.block, dims.half
    dp, rep = lax.axis_index("dp"), lax.axis_index("rep")
    f32, bf16 = jnp.float32, jnp.bfloat16
    ids = ids.reshape(1, -1)
    scale_row, shift_row = hash_scale.reshape(1, -1), hash_shift.reshape(1, -1)
    loaded = (ids, scale_row, shift_row, w_code, cotangent)
    (send,) = kernel_call(
        dims, first_kernel,
        [((dims.devices, dims.send_rows, LANES), bf16)],
        (counts,) + loaded, 1, "first", 10**9, hbm=(1, 2, 3, 4, 5),
        scratch=[pltpu.VMEM(x.shape, x.dtype) for x in loaded]
        + [pltpu.SemaphoreType.DMA((len(loaded),))], vmem=60,
    )
    recv = exchange(send)

    def of_rep(x, axis):
        shape = x.shape[:axis] + (chips, reps, block) + x.shape[axis + 1 :]
        x = lax.dynamic_index_in_dim(x.reshape(shape), rep, axis + 1, keepdims=False)
        return x.reshape(x.shape[:axis] + (half,) + x.shape[axis + 2 :])

    place, side = dp.reshape(1).astype(jnp.int32), rep.reshape(1).astype(jnp.int32)
    w_half, w_out_half = of_rep(w_code, 1), of_rep(w_out, 0)
    gain_half = of_rep(norm_gain, 0).reshape(1, -1)
    bias_half = of_rep(norm_bias, 0).reshape(1, -1)
    w_own = lax.dynamic_slice_in_dim(w_code, (dp * reps + rep) * block, block, 1)
    w_own = jnp.concatenate([w_own] * dims.groups, axis=1)
    grads, stat, all_ids, all_counts = kernel_call(
        dims, middle_kernel,
        [
            ((chips, dims.grad_rows, LANES), bf16),
            ((8, half), f32),
            ((chips, dims.devices * dims.take), f32),
            ((dims.devices, LANES), f32),
        ],
        (place, recv, w_half, gain_half, bias_half, w_out_half, scale_row, shift_row, w_own), 1,
        "middle", 10**9,
    )
    share = lax.all_to_all(grads, "dp", split_axis=0, concat_axis=0, tiled=True)

    def partner(x):
        return lax.ppermute(x, "rep", [(i, (i + 1) % reps) for i in range(reps)])

    packed = chips * dims.rows // dims.groups
    embedded, token = kernel_call(
        dims, embed_kernel, [((dims.slots, dims.width), bf16), ((8, LANES), f32)],
        (
            counts, side, ids, scale_row, shift_row,
            pltpu.with_memory_space_constraint(w_code, pltpu.HBM), stat, partner(stat),
            norm_gain.reshape(1, -1), norm_bias.reshape(1, -1),
            pltpu.with_memory_space_constraint(w_out, pltpu.HBM), out_bias.reshape(1, -1),
        ),
        2, "embed", 10**9, hbm=(5, 10),
        scratch=[
            pltpu.VMEM(w_code.shape, bf16), pltpu.VMEM(w_out.shape, bf16),
            pltpu.SemaphoreType.DMA((3,)),
        ],
    )
    fixed, *code = kernel_call(
        dims, owner_kernel,
        [((block + 8, dims.codes), f32)] + [((dims.piece, dims.codes), bf16)] * (dims.groups * dims.parts),
        (place, all_ids, all_counts, w_own, scale_row, shift_row, stat, token), 1,
        "owner", 4 * 10**9,
    )
    pair = share[:, dims.rows // dims.groups + block :, :]
    other = partner(pair)
    code_share, out_share = kernel_call(
        dims, last_kernel, [((block, dims.codes), f32), ((block, dims.width), f32)],
        (place, share, fixed, stat, gain_half, *code), 1, "last", 10**9,
    )
    gain, bias = kernel_call(
        dims, join_kernel, [((1, dims.hidden), f32)] * 2, (side, pair, other), 1, "join", 10**6
    )
    return embedded, code_share, out_share, gain.reshape(-1), bias.reshape(-1)


def solution(mesh):
    rows = P(AXES)

    def per_device(*arguments):
        ids, w_code, w_out = arguments[0], arguments[4], arguments[7]
        dims = Dims(mesh, ids.shape[0], w_code.shape[0], w_code.shape[1], w_out.shape[1])
        if dims.reps == 2 and dims.fits():
            return fast_device(dims, *arguments)
        return general_device(*arguments)

    return jax.shard_map(
        per_device,
        mesh=mesh,
        in_specs=(rows, rows, P(), P(), P(), P(), P(), P(), P(), P(AXES, None)),
        out_specs=(P(AXES, None), P(AXES, None), P(AXES, None), P(), P()),
        check_vma=False,
    )
```

```python
import functools
import math

import jax
import jax.numpy as jnp
from jax import lax
from jax.experimental import pallas as pl
from jax.experimental.pallas import tpu as pltpu
from jax.sharding import PartitionSpec as P

LANES = 128
PARTS = 4
modulus = 65521
epsilon = 1e-05
AXES = ("dp", "rep")


def hashed(ident, hash_scale, hash_shift):
    resid = ident % modulus
    bucket = (hash_scale[None, :] * resid[:, None] + hash_shift[None, :]) % modulus
    return (bucket.astype(jnp.float32) * (2.0 / (modulus - 1)) - 1.0).astype(jnp.bfloat16)


def mish_parts(gated):
    softer = jax.nn.softplus(gated)
    tangent = jnp.tanh(softer)
    return (gated * tangent, tangent + gated * (1.0 - tangent * tangent) * jax.nn.sigmoid(gated))


def exchange(blocks):
    return lax.all_to_all(blocks, AXES, split_axis=0, concat_axis=0, tiled=True)


def lane_rows(flat):
    pad = -flat.shape[-1] % (8 * LANES)
    flat = jnp.pad(flat, [(0, 0)] * (flat.ndim - 1) + [(0, pad)])
    return flat.reshape(flat.shape[:-1] + (-1, LANES))


def general_device(
    ids, counts, hash_scale, hash_shift, w_code, norm_gain, norm_bias, w_out, out_bias, cotangent
):
    devices = lax.axis_size("dp") * lax.axis_size("rep")
    me = lax.axis_index("dp") * lax.axis_size("rep") + lax.axis_index("rep")
    slots = ids.shape[0]
    codes, hidden = w_code.shape
    width = w_out.shape[1]
    share = hidden // devices
    keep = (jnp.arange(slots, dtype=jnp.int32) < counts[0])[:, None]

    preact = jnp.dot(
        hashed(ids, hash_scale, hash_shift), w_code, preferred_element_type=jnp.float32
    )
    masked = jnp.where(keep, preact, 0.0)
    row = lane_rows(
        jnp.concatenate(
            [
                masked.sum(0),
                (masked * masked).sum(0),
                ids.astype(jnp.float32),
                counts.astype(jnp.float32),
            ]
        )
    )
    table = exchange(jnp.broadcast_to(row, (devices,) + row.shape)).reshape(devices, -1)
    sums = table[:, : 2 * hidden].sum(0)
    all_ids = table[:, 2 * hidden : 2 * hidden + slots].astype(jnp.int32)
    all_counts = table[:, 2 * hidden + slots].astype(jnp.int32)
    total = all_counts.sum().astype(jnp.float32)
    mean = sums[:hidden] / total
    inv_std = lax.rsqrt(sums[hidden:] / total - mean * mean + epsilon)

    normed = (preact - mean) * inv_std
    act_full, slope = mish_parts(normed * norm_gain + norm_bias)
    act = act_full.astype(jnp.bfloat16)
    delta = jnp.where(keep, cotangent.astype(jnp.float32) * lax.rsqrt(total), 0.0).astype(
        jnp.bfloat16
    )
    dval = (
        lax.dot_general(delta, w_out, (((1,), (1,)), ((), ())), preferred_element_type=jnp.float32)
        * slope
    )
    grad_out = lax.dot_general(
        act, delta, (((0,), (0,)), ((), ())), preferred_element_type=jnp.float32
    )
    columns = exchange(dval.astype(jnp.bfloat16).T.reshape(devices, share, slots))
    pair = jnp.concatenate([(dval * normed).sum(0), dval.sum(0)])
    grads = exchange(
        lane_rows(
            jnp.concatenate(
                [
                    grad_out.reshape(devices, share * width),
                    jnp.broadcast_to(pair, (devices, 2 * hidden)),
                ],
                axis=1,
            )
        )
    )
    grads = grads.reshape(devices, -1)[:, : share * width + 2 * hidden].sum(0)
    out_share = grads[: share * width].reshape(share, width)
    grad_gain = grads[share * width : share * width + hidden]
    grad_bias = grads[share * width + hidden :]

    embedded = jnp.dot(act, w_out, preferred_element_type=jnp.float32) + out_bias
    embedded = jnp.where(keep, embedded, 0.0).astype(jnp.bfloat16)

    def own(vector):
        return lax.dynamic_slice_in_dim(vector, me * share, share, vector.ndim - 1)

    w_own = own(w_code)
    mean_own, inv_own = own(mean), own(inv_std)
    shift_own, tilt_own = own(grad_bias) / total, own(grad_gain) / total
    scale_own = own(norm_gain) * inv_own
    group = math.gcd(devices, max(1, 8192 // slots))

    def accumulate(index, grad_rows):
        start = index * group
        block_ids = lax.dynamic_slice_in_dim(all_ids, start, group, 0).reshape(-1)
        block_counts = lax.dynamic_slice_in_dim(all_counts, start, group, 0)
        block = lax.dynamic_slice_in_dim(columns, start, group, 0)
        code = hashed(block_ids, hash_scale, hash_shift)
        pre = lax.dot_general(
            w_own, code, (((0,), (1,)), ((), ())), preferred_element_type=jnp.float32
        )
        seen = (pre - mean_own[:, None]) * inv_own[:, None]
        dval_own = block.transpose(1, 0, 2).reshape(share, -1).astype(jnp.float32)
        dpre = scale_own[:, None] * (dval_own - shift_own[:, None] - seen * tilt_own[:, None])
        live = jnp.arange(slots, dtype=jnp.int32)[None, :] < block_counts[:, None]
        dpre = jnp.where(live.reshape(1, -1), dpre, 0.0).astype(jnp.bfloat16)
        return grad_rows + jnp.dot(dpre, code, preferred_element_type=jnp.float32)

    code_share = lax.fori_loop(
        0, devices // group, accumulate, jnp.zeros((share, codes), jnp.float32)
    )
    return embedded, code_share, out_share, grad_gain, grad_bias


def row_of(tiles):
    return jnp.concatenate(tiles, axis=1)


def place_block(tile, source, target, block):
    shift = ((target - source) * block) % LANES
    return pltpu.roll(tile, shift, 1) if shift else tile


def pick_blocks(x, chosen, block):
    per_tile = LANES // block
    lane = lax.broadcasted_iota(jnp.int32, (x.shape[0], LANES), 1) // block
    tiles = []
    for first in range(0, len(chosen), per_tile):
        tile = None
        for place, b in enumerate(chosen[first : first + per_tile]):
            start = b // per_tile * LANES
            piece = place_block(x[:, start : start + LANES], b % per_tile, place, block)
            tile = piece if tile is None else jnp.where(lane == place, piece, tile)
        tiles.append(tile)
    return tiles


def split_pair(x):
    high = x.astype(jnp.bfloat16).astype(jnp.float32)
    return high, (x - high).astype(jnp.bfloat16).astype(jnp.float32)


def codes_of(id_column, scale_row, shift_row):
    raw = scale_row * id_column + shift_row
    once = (raw - lax.shift_right_logical(raw, 16) * modulus).astype(jnp.float32)
    quotient = jnp.floor((once + 0.5) * (1.0 / modulus))
    bucket = once - quotient * float(modulus)
    return (bucket * (2.0 / (modulus - 1)) - 1.0).astype(jnp.bfloat16)


def mish_of(val):
    grown = jnp.exp(jnp.minimum(val, 20.0))
    n = grown * (grown + 2.0)
    inverse = 1.0 / (n + 2.0)
    t = n * inverse
    slope = t + val * (4.0 * grown * (1.0 + grown)) * (inverse * inverse)
    return val * t, slope


def dot_t(a, b):
    return lax.dot_general(a, b, (((1,), (1,)), ((), ())), preferred_element_type=jnp.float32)


def dot_rows(a, b):
    return lax.dot_general(a, b, (((0,), (0,)), ((), ())), preferred_element_type=jnp.float32)


def one_hot(condition):
    return jnp.where(condition, 1.0, 0.0).astype(jnp.bfloat16)


def id_bytes(ids_row):
    resid = lax.rem(ids_row, modulus)
    high = lax.shift_right_logical(resid, 8).astype(jnp.float32)
    low = lax.bitwise_and(resid, 255).astype(jnp.float32)
    return high, low, jnp.zeros((6, ids_row.shape[1]), jnp.float32)


def slot_codes(high, low, blank, scale_row, shift_row):
    slots = high.shape[1]
    same = one_hot(
        lax.broadcasted_iota(jnp.int32, (slots, slots), 0)
        == lax.broadcasted_iota(jnp.int32, (slots, slots), 1)
    )
    pieces = jnp.concatenate([high, low, blank], axis=0).astype(jnp.bfloat16)
    columns = dot_t(same, pieces)
    id_column = (columns[:, 0:1] * 256.0 + columns[:, 1:2]).astype(jnp.int32)
    return codes_of(id_column, scale_row, shift_row)


def first_kernel(
    dims, count_ref, _, __, ids_hbm, scale_hbm, shift_hbm, w_hbm, cot_hbm, gain_hbm, bias_hbm,
    w_out_hbm, send_ref, scale_ref, shift_ref, w_ref, gain_ref, bias_ref, w_out_ref,
    ids_ref, cot_ref, sems,
):
    chips, reps, take, block = dims.chips, dims.reps, dims.take, dims.block
    slots = dims.slots
    copies = [
        pltpu.make_async_copy(source, target, sems.at[i])
        for i, (source, target) in enumerate(
            [
                (ids_hbm, ids_ref),
                (scale_hbm, scale_ref),
                (shift_hbm, shift_ref),
                (w_hbm, w_ref),
                (cot_hbm, cot_ref),
                (gain_hbm, gain_ref),
                (bias_hbm, bias_ref),
                (w_out_hbm, w_out_ref),
            ]
        )
    ]
    for copy in copies:
        copy.start()
    count = count_ref[0]
    r = lax.broadcasted_iota(jnp.int32, (slots, slots), 0)
    c = lax.broadcasted_iota(jnp.int32, (slots, slots), 1)
    order = one_hot(c == (r % take) * chips + r // take)
    for copy in copies[:3]:
        copy.wait()
    high, low, blank = id_bytes(ids_ref[...])
    codes = slot_codes(high, low, blank, scale_ref[...], shift_ref[...])
    live = lax.broadcasted_iota(jnp.int32, (1, slots), 1) < count
    marked = jnp.concatenate([jnp.where(live, high, 256.0), low, blank], axis=0)
    by_chip = dot_t(marked.astype(jnp.bfloat16), order)
    tail = [
        by_chip[i : i + 1, t * LANES : (t + 1) * LANES]
        for i in range(2)
        for t in range(slots // LANES)
    ]
    for copy in copies[3:5]:
        copy.wait()
    pre = jnp.dot(codes, w_ref[...], preferred_element_type=jnp.float32)
    moved = jnp.dot(order, cot_ref[...], preferred_element_type=jnp.float32).astype(jnp.bfloat16)
    keep = lax.broadcasted_iota(jnp.int32, (slots, 1), 0) < count
    sums = jnp.where(keep, pre, 0.0).sum(0, keepdims=True)
    apart = jnp.where(keep, pre - sums / count.astype(jnp.float32), 0.0)
    spread = (apart * apart).sum(0, keepdims=True)
    stats = jnp.concatenate(split_pair(sums) + (spread,), axis=0)
    for rep in range(reps):
        tiles = pick_blocks(stats, [k * reps + rep for k in range(chips)], block)
        lower = jnp.concatenate(tiles + tail, axis=0).astype(jnp.bfloat16)
        for k in range(chips):
            send_ref[k * reps + rep, :take, :] = moved[k * take : (k + 1) * take, :]
            send_ref[k * reps + rep, take:, :] = lower
    for copy in copies[5:]:
        copy.wait()


def id_rows(dims, recv):
    base = dims.take + dims.stat_rows
    parts = dims.slots // LANES
    rows = dims.devices * dims.take
    spread = one_hot(
        lax.broadcasted_iota(jnp.int32, (rows, dims.devices), 0) // dims.take
        == lax.broadcasted_iota(jnp.int32, (rows, dims.devices), 1)
    )
    own_j = (
        lax.broadcasted_iota(jnp.int32, (rows, dims.slots), 1) % dims.take
        == lax.broadcasted_iota(jnp.int32, (rows, dims.slots), 0) % dims.take
    )
    fold = one_hot(
        lax.broadcasted_iota(jnp.int32, (dims.chips, dims.slots), 1) // dims.take
        == lax.broadcasted_iota(jnp.int32, (dims.chips, dims.slots), 0)
    )
    flats = [
        row_of([recv[:, base + i * parts + t, :] for t in range(parts)]) for i in range(2)
    ]
    counts = jnp.where(flats[0] < 255.5, 1.0, 0.0).sum(1, keepdims=True)
    tables = []
    for flat in flats:
        wide = jnp.dot(spread, flat.astype(jnp.bfloat16), preferred_element_type=jnp.float32)
        tables.append(dot_t(fold, jnp.where(own_j, wide, 0.0).astype(jnp.bfloat16)))
    return counts, tables[0] * 256.0 + tables[1]


def packing(dims, counts, chip):
    lanes = dims.devices * dims.take
    d = lax.broadcasted_iota(jnp.int32, (dims.devices, lanes), 0)
    l = lax.broadcasted_iota(jnp.int32, (dims.devices, lanes), 1) // dims.take
    j = (lax.broadcasted_iota(jnp.int32, (1, lanes), 1) % dims.take).astype(jnp.float32)
    live = jnp.maximum(jnp.floor((counts - chip + (dims.chips - 1.0)) * (1.0 / dims.chips)), 0.0)
    before = jnp.where(d < l, live, 0.0).sum(0, keepdims=True)
    here = jnp.where(d == l, live, 0.0).sum(0, keepdims=True)
    target = jnp.where(j < here, before + j, -1.0).astype(jnp.int32)
    return target, live.sum(0, keepdims=True)


def half_of(dims, x, rep):
    tiles = [x[:, t : t + LANES] for t in range(0, dims.hidden, LANES)]
    moved = [jnp.where(rep == 0, t, pltpu.roll(t, LANES - dims.block, 1)) for t in tiles]
    return row_of(pick_blocks(row_of(moved), [k * dims.reps for k in range(dims.chips)], dims.block))


def middle_kernel(
    dims, place_ref, side_ref, recv_ref, w_ref, gain_ref, bias_ref, w_out_ref, scale_ref, shift_ref,
    send_ref, stat_ref, ids_ref, counts_ref,
):
    take, block, rows = dims.take, dims.block, dims.rows
    half, groups = dims.half, dims.groups
    chip, rep = place_ref[0], side_ref[0]
    recv = recv_ref[:, take:, :].astype(jnp.float32)
    recv_all = jnp.concatenate([jnp.zeros((dims.devices, take, LANES), jnp.float32), recv], axis=1)
    counts, ids = id_rows(dims, recv_all)
    ids_ref[...] = ids
    counts_ref[...] = jnp.zeros((dims.devices, LANES), jnp.float32) + counts
    total = counts.sum(0, keepdims=True)
    target, _ = packing(dims, counts, chip.astype(jnp.float32))
    hit = lax.broadcasted_iota(jnp.int32, (rows, dims.devices * take), 0) == target
    own = lax.broadcasted_iota(jnp.int32, (dims.chips, 1), 0) == chip
    own_ids = jnp.where(own, ids, 0.0).sum(0, keepdims=True)
    id_column = jnp.where(hit, own_ids, 0.0).sum(1, keepdims=True).astype(jnp.int32)
    codes = codes_of(id_column, scale_ref[...], shift_ref[...])
    pre = half_of(dims, jnp.dot(codes, w_ref[...], preferred_element_type=jnp.float32), rep)
    cot = jnp.dot(
        one_hot(hit), recv_ref[:, :take, :].reshape(dims.devices * take, LANES),
        preferred_element_type=jnp.float32,
    )
    means, variances = [], []
    for t in range(half // LANES):
        r = 3 * t
        sums = recv[:, r, :] + recv[:, r + 1, :]
        mean = sums.sum(0, keepdims=True) / total
        off = sums / counts - mean
        means.append(mean)
        variances.append((recv[:, r + 2, :] + counts * (off * off)).sum(0, keepdims=True) / total)
    mean = row_of(means)
    inv_std = lax.rsqrt(row_of(variances) + epsilon)
    gain = half_of(dims, gain_ref[...], rep)
    bias = half_of(dims, bias_ref[...], rep)
    stat_ref[...] = jnp.concatenate(
        [mean, inv_std, gain, jnp.zeros((5, half), jnp.float32) + total], axis=0
    )
    w_out = jnp.concatenate(
        [
            w_out_ref[pl.ds(pl.multiple_of((k * dims.reps + rep) * block, block), block), :]
            for k in range(dims.chips)
        ],
        axis=0,
    )
    normed = (pre - mean) * inv_std
    act, slope = mish_of(normed * gain + bias)
    delta = (cot * lax.rsqrt(total)).astype(jnp.bfloat16)
    dval = dot_t(delta, w_out) * slope
    grad_out = dot_rows(act.astype(jnp.bfloat16), delta).astype(jnp.bfloat16)
    pair = [(dval * normed).sum(0, keepdims=True), dval.sum(0, keepdims=True)]
    pair = jnp.concatenate(
        [x[:, t * LANES : (t + 1) * LANES] for x in pair for t in range(half // LANES)], axis=0
    ).astype(jnp.bfloat16)
    part = rows // groups
    lane = lax.broadcasted_iota(jnp.int32, (part, LANES), 1) // block
    for k in range(dims.chips):
        start = k // groups * LANES
        tile = None
        for q in range(groups):
            piece = dval[q * part : (q + 1) * part, start : start + LANES]
            piece = place_block(piece, k % groups, q, block)
            tile = piece if tile is None else jnp.where(lane == q, piece, tile)
        send_ref[k, :part, :] = tile.astype(jnp.bfloat16)
        send_ref[k, part : part + block, :] = grad_out[k * block : (k + 1) * block, :]
        send_ref[k, part + block :, :] = pair


def natural(dims, mine, other, rep):
    groups, reps, block = dims.groups, dims.reps, dims.block
    halves = [jnp.where(rep == 0, mine, other), jnp.where(rep == 0, other, mine)]
    lane = lax.broadcasted_iota(jnp.int32, (mine.shape[0], LANES), 1) // block
    tiles = []
    for first in range(0, dims.chips * reps, groups):
        tile = None
        for place in range(groups):
            k, p = (first + place) // reps, (first + place) % reps
            start = k // groups * LANES
            piece = place_block(halves[p][:, start : start + LANES], k % groups, place, block)
            tile = piece if tile is None else jnp.where(lane == place, piece, tile)
        tiles.append(tile)
    return row_of(tiles)


def embed_kernel(
    dims, count_ref, rep_ref, ids_ref, scale_ref, shift_ref, w_hbm, mine_ref, other_ref, gain_ref,
    bias_ref, w_out_hbm, out_bias_ref, out_ref, token_ref, w_ref, w_out_ref, sems,
):
    cut = dims.codes // 2
    copies = [
        pltpu.make_async_copy(
            w_hbm.at[pl.ds(i * cut, cut)], w_ref.at[pl.ds(i * cut, cut)], sems.at[i]
        )
        for i in range(2)
    ]
    copies.append(pltpu.make_async_copy(w_out_hbm, w_out_ref, sems.at[2]))
    for copy in copies:
        copy.start()
    codes = slot_codes(*id_bytes(ids_ref[...]), scale_ref[...], shift_ref[...])
    copies[0].wait()
    pre = jnp.dot(codes[:, :cut], w_ref[:cut, :], preferred_element_type=jnp.float32)
    copies[1].wait()
    pre = pre + jnp.dot(codes[:, cut:], w_ref[cut:, :], preferred_element_type=jnp.float32)
    copies[2].wait()
    moments = natural(dims, mine_ref[...], other_ref[...], rep_ref[0])
    normed = (pre - moments[0:1, :]) * moments[1:2, :]
    act, _ = mish_of(normed * gain_ref[...] + bias_ref[...])
    out = jnp.dot(act.astype(jnp.bfloat16), w_out_ref[...], preferred_element_type=jnp.float32)
    keep = lax.broadcasted_iota(jnp.int32, (dims.slots, 1), 0) < count_ref[0]
    out_ref[...] = jnp.where(keep, out + out_bias_ref[...], 0.0).astype(jnp.bfloat16)
    token_ref[...] = jnp.zeros((8, LANES), jnp.float32)


def spread_own(dims, x, chip):
    groups, block = dims.groups, dims.block
    lane = lax.broadcasted_iota(jnp.int32, (1, LANES), 1) // block
    own = jnp.zeros((1, LANES), jnp.float32)
    for t in range(dims.half // LANES):
        own = own + jnp.where(
            lane + t * groups == chip, x[:, t * LANES : (t + 1) * LANES], 0.0
        )
    out = own
    for i in range(1, groups):
        out = out + pltpu.roll(own, i * block, 1)
    return out


def codes_of_group(dims, code_refs, q):
    return jnp.concatenate(
        [ref[...] for ref in code_refs[q * dims.parts : (q + 1) * dims.parts]], axis=0
    )


def owner_kernel(
    dims, place_ref, ids_ref, counts_ref, w_ref, scale_ref, shift_ref, stat_ref, _, fixed_ref,
    *code_refs,
):
    counts = counts_ref[:, 0:1]
    part, block, groups = dims.rows // dims.groups, dims.block, dims.groups
    chip = place_ref[0]
    mean = spread_own(dims, stat_ref[0:1, :], chip)
    inv_std = spread_own(dims, stat_ref[1:2, :], chip)
    group = lax.broadcasted_iota(jnp.int32, (part, LANES), 1) // block
    row = lax.broadcasted_iota(jnp.int32, (part, LANES), 0)
    wide = lax.broadcasted_iota(jnp.int32, (dims.rows, dims.devices * dims.take), 0)
    pieces = [[] for _ in range(groups)]
    for s in range(dims.chips):
        target, live = packing(dims, counts, float(s))
        id_column = jnp.where(wide == target, ids_ref[s : s + 1, :], 0.0).sum(1, keepdims=True)
        codes = codes_of(id_column.astype(jnp.int32), scale_ref[...], shift_ref[...])
        pre = jnp.dot(codes, w_ref[...], preferred_element_type=jnp.float32)
        for q in range(groups):
            start = s * part
            code_refs[q * dims.parts + start // dims.piece][
                start % dims.piece : start % dims.piece + part, :
            ] = codes[q * part : (q + 1) * part, :]
            normed = (pre[q * part : (q + 1) * part, :] - mean) * inv_std
            piece = jnp.where(group == q, normed, jnp.where(group == (q + 1) % groups, 1.0, 0.0))
            piece = jnp.where((q * part + row).astype(jnp.float32) < live, piece, 0.0)
            pieces[q].append(piece)
    moved, plain = None, None
    for q in range(groups):
        term = dot_rows(
            jnp.concatenate(pieces[q], axis=0).astype(jnp.bfloat16), codes_of_group(dims, code_refs, q)
        )
        after = (q + 1) % groups
        own, ones = term[q * block : (q + 1) * block, :], term[after * block : (after + 1) * block, :]
        moved = own if moved is None else moved + own
        plain = ones if plain is None else plain + ones
    fixed_ref[:block, :] = moved
    fixed_ref[block:, :] = plain[:8, :]


def pair_sums(dims, rows):
    pair = rows.astype(jnp.float32).sum(0)
    tiles = dims.half // LANES
    return [
        row_of([pair[i * tiles + t : i * tiles + t + 1, :] for t in range(tiles)]) for i in range(2)
    ]


def own_column(dims, x, chip):
    own = spread_own(dims, x, chip)
    spot = lax.broadcasted_iota(jnp.int32, (dims.block, LANES), 1)
    same = spot == lax.broadcasted_iota(jnp.int32, (dims.block, LANES), 0)
    return jnp.where(same, own, 0.0).sum(1, keepdims=True)


def last_kernel(
    dims, place_ref, recv_ref, fixed_ref, stat_ref, *refs
):
    part, block, groups = dims.rows // dims.groups, dims.block, dims.groups
    code_refs, (code_out_ref, out_out_ref) = refs[:-2], refs[-2:]
    chip = place_ref[0]
    total = stat_ref[3:4, :1]
    scale = own_column(dims, stat_ref[2:3, :] * stat_ref[1:2, :], chip)
    gain, bias = pair_sums(dims, recv_ref[:, part + block :, :])
    tilt = own_column(dims, gain, chip) / total
    shift = own_column(dims, bias, chip) / total
    out_out_ref[...] = recv_ref[:, part : part + block, :].astype(jnp.float32).sum(0)
    dval = recv_ref[:, :part, :].reshape(dims.chips * part, LANES)
    out = -(shift * fixed_ref[block : block + 1, :] + tilt * fixed_ref[:block, :])
    for q in range(groups):
        out = out + dot_rows(dval, codes_of_group(dims, code_refs, q))[q * block : (q + 1) * block, :]
    code_out_ref[...] = scale * out


def join_kernel(dims, rep_ref, mine_ref, other_ref, gain_ref, bias_ref):
    blank = jnp.zeros((6, dims.half), jnp.float32)
    mine, other = (
        jnp.concatenate(pair_sums(dims, ref[...]) + [blank], axis=0) for ref in (mine_ref, other_ref)
    )
    pair = natural(dims, mine, other, rep_ref[0])
    gain_ref[...] = pair[0:1, :]
    bias_ref[...] = pair[1:2, :]


class Dims:
    def __init__(self, mesh, slots, codes, hidden, width):
        self.chips, self.reps = mesh.shape["dp"], mesh.shape["rep"]
        self.devices = self.chips * self.reps
        self.slots, self.codes, self.hidden, self.width = slots, codes, hidden, width
        self.block = hidden // self.devices
        self.half = hidden // self.reps
        self.groups = LANES // max(1, self.block)
        self.take = slots // self.chips
        self.parts = PARTS
        bound = self.devices * slots // 4 // self.chips
        bound += self.devices * (self.chips - 1) // self.chips
        step = 8 * self.groups
        self.rows = min(-(-bound // step) * step, self.devices * self.take)
        self.piece = self.chips * self.rows // self.groups // self.parts
        self.stat_rows = 3 * self.half // LANES
        self.send_rows = self.take + self.stat_rows + 2 * slots // LANES
        self.grad_rows = self.rows // self.groups + self.block + 2 * self.half // LANES

    def fits(self):
        return (
            self.width == LANES
            and LANES % self.block == 0
            and self.block % 8 == 0
            and self.chips % self.parts == 0
            and self.take % 8 == 0
            and self.slots % LANES == 0
            and self.half % LANES == 0
            and self.codes % LANES == 0
            and self.chips <= LANES
            and self.slots <= 256
            and self.rows % (8 * self.groups) == 0
            and self.chips * self.rows * self.codes <= (1 << 22)
        )


def kernel_call(dims, body, outs, arguments, scalars, name, flops, hbm=(), scratch=(), vmem=16):
    specs = [pl.BlockSpec(memory_space=pltpu.SMEM)] * scalars
    for i in range(scalars, len(arguments)):
        specs.append(pl.BlockSpec(memory_space=pltpu.HBM if i in hbm else pltpu.VMEM))
    return pl.pallas_call(
        functools.partial(body, dims),
        out_shape=[jax.ShapeDtypeStruct(shape, kind) for shape, kind in outs],
        in_specs=specs,
        out_specs=[pl.BlockSpec(memory_space=pltpu.VMEM)] * len(outs),
        scratch_shapes=list(scratch),
        compiler_params=pltpu.CompilerParams(vmem_limit_bytes=vmem << 20),
        cost_estimate=pl.CostEstimate(flops=flops, bytes_accessed=1 << 20, transcendentals=0),
        name=name,
    )(*arguments)


def fast_device(
    dims, ids, counts, hash_scale, hash_shift, w_code, norm_gain, norm_bias, w_out, out_bias,
    cotangent,
):
    chips, reps, block, half = dims.chips, dims.reps, dims.block, dims.half
    dp, rep = lax.axis_index("dp"), lax.axis_index("rep")
    f32, bf16 = jnp.float32, jnp.bfloat16
    place, side = dp.reshape(1).astype(jnp.int32), rep.reshape(1).astype(jnp.int32)
    ids = ids.reshape(1, -1)
    scale_row, shift_row = hash_scale.reshape(1, -1), hash_shift.reshape(1, -1)
    gain_row, bias_row = norm_gain.reshape(1, -1), norm_bias.reshape(1, -1)
    kept = (scale_row, shift_row, w_code, gain_row, bias_row, w_out)
    loaded = (ids, scale_row, shift_row, w_code, cotangent, gain_row, bias_row, w_out)
    send, scale_row, shift_row, w_near, gain_row, bias_row, w_out_near = kernel_call(
        dims, first_kernel,
        [((dims.devices, dims.send_rows, LANES), bf16)]
        + [(x.shape, x.dtype) for x in kept],
        (counts, place, side) + tuple(pltpu.with_memory_space_constraint(x, pltpu.HBM) for x in loaded),
        3, "first", 10**9, hbm=range(3, 3 + len(loaded)),
        scratch=[pltpu.VMEM(x.shape, x.dtype) for x in (ids, cotangent)]
        + [pltpu.SemaphoreType.DMA((len(loaded),))],
    )
    recv = exchange(send)

    grads, stat, all_ids, all_counts = kernel_call(
        dims, middle_kernel,
        [
            ((chips, dims.grad_rows, LANES), bf16),
            ((8, half), f32),
            ((chips, dims.devices * dims.take), f32),
            ((dims.devices, LANES), f32),
        ],
        (
            place, side, recv, w_near, gain_row, bias_row, w_out_near, scale_row, shift_row,
        ),
        2,
        "middle", 10**9,
    )
    share = lax.all_to_all(grads, "dp", split_axis=0, concat_axis=0, tiled=True)

    def partner(x):
        return lax.ppermute(x, "rep", [(i, (i + 1) % reps) for i in range(reps)])

    w_own, stat, at, of = lax.optimization_barrier((w_code, stat, place, side))
    w_own = lax.dynamic_slice_in_dim(w_own, (at[0] * reps + of[0]) * block, block, 1)
    w_own = jnp.concatenate([w_own] * dims.groups, axis=1)
    packed = chips * dims.rows // dims.groups
    embedded, token = kernel_call(
        dims, embed_kernel, [((dims.slots, dims.width), bf16), ((8, LANES), f32)],
        (
            counts, side, ids, scale_row, shift_row,
            pltpu.with_memory_space_constraint(w_code, pltpu.HBM), stat, partner(stat),
            gain_row, bias_row,
            pltpu.with_memory_space_constraint(w_out, pltpu.HBM), out_bias.reshape(1, -1),
        ),
        2, "embed", 10**9, hbm=(5, 10),
        scratch=[
            pltpu.VMEM(w_code.shape, bf16), pltpu.VMEM(w_out.shape, bf16),
            pltpu.SemaphoreType.DMA((3,)),
        ],
    )
    fixed, *code = kernel_call(
        dims, owner_kernel,
        [((block + 8, dims.codes), f32)] + [((dims.piece, dims.codes), bf16)] * (dims.groups * dims.parts),
        (place, all_ids, all_counts, w_own, scale_row, shift_row, stat, token), 1,
        "owner", 4 * 10**9,
    )
    pair = share[:, dims.rows // dims.groups + block :, :]
    other = partner(pair)
    code_share, out_share = kernel_call(
        dims, last_kernel, [((block, dims.codes), f32), ((block, dims.width), f32)],
        (place, share, fixed, stat, *code), 1, "last", 10**9,
    )
    gain, bias = kernel_call(
        dims, join_kernel, [((1, dims.hidden), f32)] * 2, (side, pair, other), 1, "join", 10**6
    )
    return embedded, code_share, out_share, gain.reshape(-1), bias.reshape(-1)


def solution(mesh):
    rows = P(AXES)

    def per_device(*arguments):
        ids, w_code, w_out = arguments[0], arguments[4], arguments[7]
        dims = Dims(mesh, ids.shape[0], w_code.shape[0], w_code.shape[1], w_out.shape[1])
        if dims.reps == 2 and dims.fits():
            return fast_device(dims, *arguments)
        return general_device(*arguments)

    return jax.shard_map(
        per_device,
        mesh=mesh,
        in_specs=(rows, rows, P(), P(), P(), P(), P(), P(), P(), P(AXES, None)),
        out_specs=(P(AXES, None), P(AXES, None), P(AXES, None), P(), P()),
        check_vma=False,
    )
```

```python
import functools
import math

import jax
import jax.numpy as jnp
from jax import lax
from jax.experimental import pallas as pl
from jax.experimental.pallas import tpu as pltpu
from jax.sharding import PartitionSpec as P

LANES = 128
PARTS = 4
modulus = 65521
epsilon = 1e-05
AXES = ("dp", "rep")


def hashed(ident, hash_scale, hash_shift):
    resid = ident % modulus
    bucket = (hash_scale[None, :] * resid[:, None] + hash_shift[None, :]) % modulus
    return (bucket.astype(jnp.float32) * (2.0 / (modulus - 1)) - 1.0).astype(jnp.bfloat16)


def mish_parts(gated):
    softer = jax.nn.softplus(gated)
    tangent = jnp.tanh(softer)
    return (gated * tangent, tangent + gated * (1.0 - tangent * tangent) * jax.nn.sigmoid(gated))


def exchange(blocks):
    return lax.all_to_all(blocks, AXES, split_axis=0, concat_axis=0, tiled=True)


def lane_rows(flat):
    pad = -flat.shape[-1] % (8 * LANES)
    flat = jnp.pad(flat, [(0, 0)] * (flat.ndim - 1) + [(0, pad)])
    return flat.reshape(flat.shape[:-1] + (-1, LANES))


def general_device(
    ids, counts, hash_scale, hash_shift, w_code, norm_gain, norm_bias, w_out, out_bias, cotangent
):
    devices = lax.axis_size("dp") * lax.axis_size("rep")
    me = lax.axis_index("dp") * lax.axis_size("rep") + lax.axis_index("rep")
    slots = ids.shape[0]
    codes, hidden = w_code.shape
    width = w_out.shape[1]
    share = hidden // devices
    keep = (jnp.arange(slots, dtype=jnp.int32) < counts[0])[:, None]

    preact = jnp.dot(
        hashed(ids, hash_scale, hash_shift), w_code, preferred_element_type=jnp.float32
    )
    masked = jnp.where(keep, preact, 0.0)
    row = lane_rows(
        jnp.concatenate(
            [
                masked.sum(0),
                (masked * masked).sum(0),
                ids.astype(jnp.float32),
                counts.astype(jnp.float32),
            ]
        )
    )
    table = exchange(jnp.broadcast_to(row, (devices,) + row.shape)).reshape(devices, -1)
    sums = table[:, : 2 * hidden].sum(0)
    all_ids = table[:, 2 * hidden : 2 * hidden + slots].astype(jnp.int32)
    all_counts = table[:, 2 * hidden + slots].astype(jnp.int32)
    total = all_counts.sum().astype(jnp.float32)
    mean = sums[:hidden] / total
    inv_std = lax.rsqrt(sums[hidden:] / total - mean * mean + epsilon)

    normed = (preact - mean) * inv_std
    act_full, slope = mish_parts(normed * norm_gain + norm_bias)
    act = act_full.astype(jnp.bfloat16)
    delta = jnp.where(keep, cotangent.astype(jnp.float32) * lax.rsqrt(total), 0.0).astype(
        jnp.bfloat16
    )
    dval = (
        lax.dot_general(delta, w_out, (((1,), (1,)), ((), ())), preferred_element_type=jnp.float32)
        * slope
    )
    grad_out = lax.dot_general(
        act, delta, (((0,), (0,)), ((), ())), preferred_element_type=jnp.float32
    )
    columns = exchange(dval.astype(jnp.bfloat16).T.reshape(devices, share, slots))
    pair = jnp.concatenate([(dval * normed).sum(0), dval.sum(0)])
    grads = exchange(
        lane_rows(
            jnp.concatenate(
                [
                    grad_out.reshape(devices, share * width),
                    jnp.broadcast_to(pair, (devices, 2 * hidden)),
                ],
                axis=1,
            )
        )
    )
    grads = grads.reshape(devices, -1)[:, : share * width + 2 * hidden].sum(0)
    out_share = grads[: share * width].reshape(share, width)
    grad_gain = grads[share * width : share * width + hidden]
    grad_bias = grads[share * width + hidden :]

    embedded = jnp.dot(act, w_out, preferred_element_type=jnp.float32) + out_bias
    embedded = jnp.where(keep, embedded, 0.0).astype(jnp.bfloat16)

    def own(vector):
        return lax.dynamic_slice_in_dim(vector, me * share, share, vector.ndim - 1)

    w_own = own(w_code)
    mean_own, inv_own = own(mean), own(inv_std)
    shift_own, tilt_own = own(grad_bias) / total, own(grad_gain) / total
    scale_own = own(norm_gain) * inv_own
    group = math.gcd(devices, max(1, 8192 // slots))

    def accumulate(index, grad_rows):
        start = index * group
        block_ids = lax.dynamic_slice_in_dim(all_ids, start, group, 0).reshape(-1)
        block_counts = lax.dynamic_slice_in_dim(all_counts, start, group, 0)
        block = lax.dynamic_slice_in_dim(columns, start, group, 0)
        code = hashed(block_ids, hash_scale, hash_shift)
        pre = lax.dot_general(
            w_own, code, (((0,), (1,)), ((), ())), preferred_element_type=jnp.float32
        )
        seen = (pre - mean_own[:, None]) * inv_own[:, None]
        dval_own = block.transpose(1, 0, 2).reshape(share, -1).astype(jnp.float32)
        dpre = scale_own[:, None] * (dval_own - shift_own[:, None] - seen * tilt_own[:, None])
        live = jnp.arange(slots, dtype=jnp.int32)[None, :] < block_counts[:, None]
        dpre = jnp.where(live.reshape(1, -1), dpre, 0.0).astype(jnp.bfloat16)
        return grad_rows + jnp.dot(dpre, code, preferred_element_type=jnp.float32)

    code_share = lax.fori_loop(
        0, devices // group, accumulate, jnp.zeros((share, codes), jnp.float32)
    )
    return embedded, code_share, out_share, grad_gain, grad_bias


def row_of(tiles):
    return jnp.concatenate(tiles, axis=1)


def place_block(tile, source, target, block):
    shift = ((target - source) * block) % LANES
    return pltpu.roll(tile, shift, 1) if shift else tile


def pick_blocks(x, chosen, block):
    per_tile = LANES // block
    lane = lax.broadcasted_iota(jnp.int32, (x.shape[0], LANES), 1) // block
    tiles = []
    for first in range(0, len(chosen), per_tile):
        tile = None
        for place, b in enumerate(chosen[first : first + per_tile]):
            start = b // per_tile * LANES
            piece = place_block(x[:, start : start + LANES], b % per_tile, place, block)
            tile = piece if tile is None else jnp.where(lane == place, piece, tile)
        tiles.append(tile)
    return tiles


def split_pair(x):
    high = x.astype(jnp.bfloat16).astype(jnp.float32)
    return high, (x - high).astype(jnp.bfloat16).astype(jnp.float32)


def codes_of(id_column, scale_row, shift_row):
    raw = scale_row * id_column + shift_row
    once = (raw - lax.shift_right_logical(raw, 16) * modulus).astype(jnp.float32)
    quotient = jnp.floor((once + 0.5) * (1.0 / modulus))
    bucket = once - quotient * float(modulus)
    return (bucket * (2.0 / (modulus - 1)) - 1.0).astype(jnp.bfloat16)


def mish_of(val):
    grown = jnp.exp(jnp.minimum(val, 20.0))
    n = grown * (grown + 2.0)
    inverse = 1.0 / (n + 2.0)
    t = n * inverse
    slope = t + val * (4.0 * grown * (1.0 + grown)) * (inverse * inverse)
    return val * t, slope


def dot_t(a, b):
    return lax.dot_general(a, b, (((1,), (1,)), ((), ())), preferred_element_type=jnp.float32)


def dot_rows(a, b):
    return lax.dot_general(a, b, (((0,), (0,)), ((), ())), preferred_element_type=jnp.float32)


def one_hot(condition):
    return jnp.where(condition, 1.0, 0.0).astype(jnp.bfloat16)


def id_bytes(ids_row):
    resid = lax.rem(ids_row, modulus)
    high = lax.shift_right_logical(resid, 8).astype(jnp.float32)
    low = lax.bitwise_and(resid, 255).astype(jnp.float32)
    return high, low, jnp.zeros((6, ids_row.shape[1]), jnp.float32)


def slot_codes(high, low, blank, scale_row, shift_row):
    slots = high.shape[1]
    same = one_hot(
        lax.broadcasted_iota(jnp.int32, (slots, slots), 0)
        == lax.broadcasted_iota(jnp.int32, (slots, slots), 1)
    )
    pieces = jnp.concatenate([high, low, blank], axis=0).astype(jnp.bfloat16)
    columns = dot_t(same, pieces)
    id_column = (columns[:, 0:1] * 256.0 + columns[:, 1:2]).astype(jnp.int32)
    return codes_of(id_column, scale_row, shift_row)


def first_kernel(
    dims, count_ref, _, __, ids_hbm, scale_hbm, shift_hbm, w_hbm, cot_hbm, gain_hbm, bias_hbm,
    w_out_hbm, send_ref, scale_ref, shift_ref, w_ref, gain_ref, bias_ref, w_out_ref,
    ids_ref, cot_ref, sems,
):
    chips, reps, take, block = dims.chips, dims.reps, dims.take, dims.block
    slots = dims.slots
    copies = [
        pltpu.make_async_copy(source, target, sems.at[i])
        for i, (source, target) in enumerate(
            [
                (ids_hbm, ids_ref),
                (scale_hbm, scale_ref),
                (shift_hbm, shift_ref),
                (w_hbm, w_ref),
                (cot_hbm, cot_ref),
                (gain_hbm, gain_ref),
                (bias_hbm, bias_ref),
                (w_out_hbm, w_out_ref),
            ]
        )
    ]
    for copy in copies:
        copy.start()
    count = count_ref[0]
    r = lax.broadcasted_iota(jnp.int32, (slots, slots), 0)
    c = lax.broadcasted_iota(jnp.int32, (slots, slots), 1)
    order = one_hot(c == (r % take) * chips + r // take)
    for copy in copies[:3]:
        copy.wait()
    high, low, blank = id_bytes(ids_ref[...])
    codes = slot_codes(high, low, blank, scale_ref[...], shift_ref[...])
    live = lax.broadcasted_iota(jnp.int32, (1, slots), 1) < count
    marked = jnp.concatenate([jnp.where(live, high, 256.0), low, blank], axis=0)
    by_chip = dot_t(marked.astype(jnp.bfloat16), order)
    tail = [
        by_chip[i : i + 1, t * LANES : (t + 1) * LANES]
        for i in range(2)
        for t in range(slots // LANES)
    ]
    for copy in copies[3:5]:
        copy.wait()
    pre = jnp.dot(codes, w_ref[...], preferred_element_type=jnp.float32)
    moved = jnp.dot(order, cot_ref[...], preferred_element_type=jnp.float32).astype(jnp.bfloat16)
    keep = lax.broadcasted_iota(jnp.int32, (slots, 1), 0) < count
    sums = jnp.where(keep, pre, 0.0).sum(0, keepdims=True)
    apart = jnp.where(keep, pre - sums / count.astype(jnp.float32), 0.0)
    spread = (apart * apart).sum(0, keepdims=True)
    stats = jnp.concatenate(split_pair(sums) + (spread,), axis=0)
    for rep in range(reps):
        tiles = pick_blocks(stats, [k * reps + rep for k in range(chips)], block)
        lower = jnp.concatenate(tiles + tail, axis=0).astype(jnp.bfloat16)
        for k in range(chips):
            send_ref[k * reps + rep, :take, :] = moved[k * take : (k + 1) * take, :]
            send_ref[k * reps + rep, take:, :] = lower
    for copy in copies[5:]:
        copy.wait()


def id_rows(dims, recv):
    base = dims.take + dims.stat_rows
    parts = dims.slots // LANES
    rows = dims.devices * dims.take
    spread = one_hot(
        lax.broadcasted_iota(jnp.int32, (rows, dims.devices), 0) // dims.take
        == lax.broadcasted_iota(jnp.int32, (rows, dims.devices), 1)
    )
    own_j = (
        lax.broadcasted_iota(jnp.int32, (rows, dims.slots), 1) % dims.take
        == lax.broadcasted_iota(jnp.int32, (rows, dims.slots), 0) % dims.take
    )
    fold = one_hot(
        lax.broadcasted_iota(jnp.int32, (dims.chips, dims.slots), 1) // dims.take
        == lax.broadcasted_iota(jnp.int32, (dims.chips, dims.slots), 0)
    )
    flats = [
        row_of([recv[:, base + i * parts + t, :] for t in range(parts)]) for i in range(2)
    ]
    counts = jnp.where(flats[0] < 255.5, 1.0, 0.0).sum(1, keepdims=True)
    tables = []
    for flat in flats:
        wide = jnp.dot(spread, flat.astype(jnp.bfloat16), preferred_element_type=jnp.float32)
        tables.append(dot_t(fold, jnp.where(own_j, wide, 0.0).astype(jnp.bfloat16)))
    return counts, tables[0] * 256.0 + tables[1]


def packing(dims, counts, chip):
    lanes = dims.devices * dims.take
    d = lax.broadcasted_iota(jnp.int32, (dims.devices, lanes), 0)
    l = lax.broadcasted_iota(jnp.int32, (dims.devices, lanes), 1) // dims.take
    j = (lax.broadcasted_iota(jnp.int32, (1, lanes), 1) % dims.take).astype(jnp.float32)
    live = jnp.maximum(jnp.floor((counts - chip + (dims.chips - 1.0)) * (1.0 / dims.chips)), 0.0)
    before = jnp.where(d < l, live, 0.0).sum(0, keepdims=True)
    here = jnp.where(d == l, live, 0.0).sum(0, keepdims=True)
    target = jnp.where(j < here, before + j, -1.0).astype(jnp.int32)
    return target, live.sum(0, keepdims=True)


def half_of(dims, x, rep):
    groups, block = dims.groups, dims.block
    lane = lax.broadcasted_iota(jnp.int32, (x.shape[0], LANES), 1) // block
    tiles = []
    for first in range(0, dims.chips, groups):
        tile = None
        for place in range(groups):
            b = (first + place) * dims.reps
            start = b // groups * LANES
            shift = lax.rem((place - b % groups - rep) * block + 2 * LANES, LANES)
            piece = pltpu.roll(x[:, start : start + LANES], shift, 1)
            tile = piece if tile is None else jnp.where(lane == place, piece, tile)
        tiles.append(tile)
    return row_of(tiles)


def middle_kernel(
    dims, place_ref, side_ref, recv_ref, w_ref, gain_ref, bias_ref, w_out_ref, scale_ref, shift_ref,
    send_ref, stat_ref, ids_ref, counts_ref,
):
    take, block, rows = dims.take, dims.block, dims.rows
    half, groups = dims.half, dims.groups
    chip, rep = place_ref[0], side_ref[0]
    recv = recv_ref[:, take:, :].astype(jnp.float32)
    recv_all = jnp.concatenate([jnp.zeros((dims.devices, take, LANES), jnp.float32), recv], axis=1)
    counts, ids = id_rows(dims, recv_all)
    ids_ref[...] = ids
    counts_ref[...] = jnp.zeros((dims.devices, LANES), jnp.float32) + counts
    total = counts.sum(0, keepdims=True)
    target, _ = packing(dims, counts, chip.astype(jnp.float32))
    hit = lax.broadcasted_iota(jnp.int32, (rows, dims.devices * take), 0) == target
    own = lax.broadcasted_iota(jnp.int32, (dims.chips, 1), 0) == chip
    own_ids = jnp.where(own, ids, 0.0).sum(0, keepdims=True)
    id_column = jnp.where(hit, own_ids, 0.0).sum(1, keepdims=True).astype(jnp.int32)
    codes = codes_of(id_column, scale_ref[...], shift_ref[...])
    pre = half_of(dims, jnp.dot(codes, w_ref[...], preferred_element_type=jnp.float32), rep)
    cot = jnp.dot(
        one_hot(hit), recv_ref[:, :take, :].reshape(dims.devices * take, LANES),
        preferred_element_type=jnp.float32,
    )
    means, variances = [], []
    for t in range(half // LANES):
        r = 3 * t
        sums = recv[:, r, :] + recv[:, r + 1, :]
        mean = sums.sum(0, keepdims=True) / total
        off = sums / counts - mean
        means.append(mean)
        variances.append((recv[:, r + 2, :] + counts * (off * off)).sum(0, keepdims=True) / total)
    mean = row_of(means)
    inv_std = lax.rsqrt(row_of(variances) + epsilon)
    gain = half_of(dims, gain_ref[...], rep)
    bias = half_of(dims, bias_ref[...], rep)
    stat_ref[...] = jnp.concatenate(
        [mean, inv_std, gain, jnp.zeros((5, half), jnp.float32) + total], axis=0
    )
    w_out = jnp.concatenate(
        [
            w_out_ref[pl.ds(pl.multiple_of((k * dims.reps + rep) * block, block), block), :]
            for k in range(dims.chips)
        ],
        axis=0,
    )
    normed = (pre - mean) * inv_std
    act, slope = mish_of(normed * gain + bias)
    delta = (cot * lax.rsqrt(total)).astype(jnp.bfloat16)
    dval = dot_t(delta, w_out) * slope
    grad_out = dot_rows(act.astype(jnp.bfloat16), delta).astype(jnp.bfloat16)
    pair = [(dval * normed).sum(0, keepdims=True), dval.sum(0, keepdims=True)]
    pair = jnp.concatenate(
        [x[:, t * LANES : (t + 1) * LANES] for x in pair for t in range(half // LANES)], axis=0
    ).astype(jnp.bfloat16)
    part = rows // groups
    lane = lax.broadcasted_iota(jnp.int32, (part, LANES), 1) // block
    for k in range(dims.chips):
        start = k // groups * LANES
        tile = None
        for q in range(groups):
            piece = dval[q * part : (q + 1) * part, start : start + LANES]
            piece = place_block(piece, k % groups, q, block)
            tile = piece if tile is None else jnp.where(lane == q, piece, tile)
        send_ref[k, :part, :] = tile.astype(jnp.bfloat16)
        send_ref[k, part : part + block, :] = grad_out[k * block : (k + 1) * block, :]
        send_ref[k, part + block :, :] = pair


def natural(dims, mine, other, rep):
    groups, reps, block = dims.groups, dims.reps, dims.block
    halves = [jnp.where(rep == 0, mine, other), jnp.where(rep == 0, other, mine)]
    lane = lax.broadcasted_iota(jnp.int32, (mine.shape[0], LANES), 1) // block
    tiles = []
    for first in range(0, dims.chips * reps, groups):
        tile = None
        for place in range(groups):
            k, p = (first + place) // reps, (first + place) % reps
            start = k // groups * LANES
            piece = place_block(halves[p][:, start : start + LANES], k % groups, place, block)
            tile = piece if tile is None else jnp.where(lane == place, piece, tile)
        tiles.append(tile)
    return row_of(tiles)


def embed_kernel(
    dims, count_ref, rep_ref, ids_ref, scale_ref, shift_ref, w_hbm, mine_ref, other_ref, gain_ref,
    bias_ref, w_out_hbm, out_bias_ref, out_ref, token_ref, w_ref, w_out_ref, sems,
):
    cut = dims.codes // 2
    copies = [
        pltpu.make_async_copy(
            w_hbm.at[pl.ds(i * cut, cut)], w_ref.at[pl.ds(i * cut, cut)], sems.at[i]
        )
        for i in range(2)
    ]
    copies.append(pltpu.make_async_copy(w_out_hbm, w_out_ref, sems.at[2]))
    for copy in copies:
        copy.start()
    codes = slot_codes(*id_bytes(ids_ref[...]), scale_ref[...], shift_ref[...])
    copies[0].wait()
    pre = jnp.dot(codes[:, :cut], w_ref[:cut, :], preferred_element_type=jnp.float32)
    copies[1].wait()
    pre = pre + jnp.dot(codes[:, cut:], w_ref[cut:, :], preferred_element_type=jnp.float32)
    copies[2].wait()
    moments = natural(dims, mine_ref[...], other_ref[...], rep_ref[0])
    normed = (pre - moments[0:1, :]) * moments[1:2, :]
    act, _ = mish_of(normed * gain_ref[...] + bias_ref[...])
    out = jnp.dot(act.astype(jnp.bfloat16), w_out_ref[...], preferred_element_type=jnp.float32)
    keep = lax.broadcasted_iota(jnp.int32, (dims.slots, 1), 0) < count_ref[0]
    out_ref[...] = jnp.where(keep, out + out_bias_ref[...], 0.0).astype(jnp.bfloat16)
    token_ref[...] = jnp.zeros((8, LANES), jnp.float32)


def spread_own(dims, x, chip):
    groups, block = dims.groups, dims.block
    lane = lax.broadcasted_iota(jnp.int32, (1, LANES), 1) // block
    own = jnp.zeros((1, LANES), jnp.float32)
    for t in range(dims.half // LANES):
        own = own + jnp.where(
            lane + t * groups == chip, x[:, t * LANES : (t + 1) * LANES], 0.0
        )
    out = own
    for i in range(1, groups):
        out = out + pltpu.roll(own, i * block, 1)
    return out


def codes_of_group(dims, code_refs, q):
    return jnp.concatenate(
        [ref[...] for ref in code_refs[q * dims.parts : (q + 1) * dims.parts]], axis=0
    )


def owner_kernel(
    dims, place_ref, ids_ref, counts_ref, w_ref, scale_ref, shift_ref, stat_ref, _, fixed_ref,
    *code_refs,
):
    counts = counts_ref[:, 0:1]
    part, block, groups = dims.rows // dims.groups, dims.block, dims.groups
    chip = place_ref[0]
    mean = spread_own(dims, stat_ref[0:1, :], chip)
    inv_std = spread_own(dims, stat_ref[1:2, :], chip)
    group = lax.broadcasted_iota(jnp.int32, (part, LANES), 1) // block
    row = lax.broadcasted_iota(jnp.int32, (part, LANES), 0)
    wide = lax.broadcasted_iota(jnp.int32, (dims.rows, dims.devices * dims.take), 0)
    pieces = [[] for _ in range(groups)]
    for s in range(dims.chips):
        target, live = packing(dims, counts, float(s))
        id_column = jnp.where(wide == target, ids_ref[s : s + 1, :], 0.0).sum(1, keepdims=True)
        codes = codes_of(id_column.astype(jnp.int32), scale_ref[...], shift_ref[...])
        pre = jnp.dot(codes, w_ref[...], preferred_element_type=jnp.float32)
        for q in range(groups):
            start = s * part
            code_refs[q * dims.parts + start // dims.piece][
                start % dims.piece : start % dims.piece + part, :
            ] = codes[q * part : (q + 1) * part, :]
            normed = (pre[q * part : (q + 1) * part, :] - mean) * inv_std
            piece = jnp.where(group == q, normed, jnp.where(group == (q + 1) % groups, 1.0, 0.0))
            piece = jnp.where((q * part + row).astype(jnp.float32) < live, piece, 0.0)
            pieces[q].append(piece)
    moved, plain = None, None
    for q in range(groups):
        term = dot_rows(
            jnp.concatenate(pieces[q], axis=0).astype(jnp.bfloat16), codes_of_group(dims, code_refs, q)
        )
        after = (q + 1) % groups
        own, ones = term[q * block : (q + 1) * block, :], term[after * block : (after + 1) * block, :]
        moved = own if moved is None else moved + own
        plain = ones if plain is None else plain + ones
    fixed_ref[:block, :] = moved
    fixed_ref[block:, :] = plain[:8, :]


def pair_sums(dims, rows):
    pair = rows.astype(jnp.float32).sum(0)
    tiles = dims.half // LANES
    return [
        row_of([pair[i * tiles + t : i * tiles + t + 1, :] for t in range(tiles)]) for i in range(2)
    ]


def own_column(dims, x, chip):
    own = spread_own(dims, x, chip)
    spot = lax.broadcasted_iota(jnp.int32, (dims.block, LANES), 1)
    same = spot == lax.broadcasted_iota(jnp.int32, (dims.block, LANES), 0)
    return jnp.where(same, own, 0.0).sum(1, keepdims=True)


def last_kernel(
    dims, place_ref, recv_ref, fixed_ref, stat_ref, *refs
):
    part, block, groups = dims.rows // dims.groups, dims.block, dims.groups
    code_refs, (code_out_ref, out_out_ref) = refs[:-2], refs[-2:]
    chip = place_ref[0]
    total = stat_ref[3:4, :1]
    scale = own_column(dims, stat_ref[2:3, :] * stat_ref[1:2, :], chip)
    gain, bias = pair_sums(dims, recv_ref[:, part + block :, :])
    tilt = own_column(dims, gain, chip) / total
    shift = own_column(dims, bias, chip) / total
    out_out_ref[...] = recv_ref[:, part : part + block, :].astype(jnp.float32).sum(0)
    dval = recv_ref[:, :part, :].reshape(dims.chips * part, LANES)
    out = -(shift * fixed_ref[block : block + 1, :] + tilt * fixed_ref[:block, :])
    for q in range(groups):
        out = out + dot_rows(dval, codes_of_group(dims, code_refs, q))[q * block : (q + 1) * block, :]
    code_out_ref[...] = scale * out


def join_kernel(dims, rep_ref, mine_ref, other_ref, gain_ref, bias_ref):
    blank = jnp.zeros((6, dims.half), jnp.float32)
    mine, other = (
        jnp.concatenate(pair_sums(dims, ref[...]) + [blank], axis=0) for ref in (mine_ref, other_ref)
    )
    pair = natural(dims, mine, other, rep_ref[0])
    gain_ref[...] = pair[0:1, :]
    bias_ref[...] = pair[1:2, :]


class Dims:
    def __init__(self, mesh, slots, codes, hidden, width):
        self.chips, self.reps = mesh.shape["dp"], mesh.shape["rep"]
        self.devices = self.chips * self.reps
        self.slots, self.codes, self.hidden, self.width = slots, codes, hidden, width
        self.block = hidden // self.devices
        self.half = hidden // self.reps
        self.groups = LANES // max(1, self.block)
        self.take = slots // self.chips
        self.parts = PARTS
        bound = self.devices * slots // 4 // self.chips
        bound += self.devices * (self.chips - 1) // self.chips
        step = 8 * self.groups
        self.rows = min(-(-bound // step) * step, self.devices * self.take)
        self.piece = self.chips * self.rows // self.groups // self.parts
        self.stat_rows = 3 * self.half // LANES
        self.send_rows = self.take + self.stat_rows + 2 * slots // LANES
        self.grad_rows = self.rows // self.groups + self.block + 2 * self.half // LANES

    def fits(self):
        return (
            self.width == LANES
            and LANES % self.block == 0
            and self.block % 8 == 0
            and self.chips % self.parts == 0
            and self.take % 8 == 0
            and self.slots % LANES == 0
            and self.half % LANES == 0
            and self.codes % LANES == 0
            and self.chips <= LANES
            and self.slots <= 256
            and self.rows % (8 * self.groups) == 0
            and self.chips * self.rows * self.codes <= (1 << 22)
        )


def kernel_call(dims, body, outs, arguments, scalars, name, flops, hbm=(), scratch=(), vmem=16):
    specs = [pl.BlockSpec(memory_space=pltpu.SMEM)] * scalars
    for i in range(scalars, len(arguments)):
        specs.append(pl.BlockSpec(memory_space=pltpu.HBM if i in hbm else pltpu.VMEM))
    return pl.pallas_call(
        functools.partial(body, dims),
        out_shape=[jax.ShapeDtypeStruct(shape, kind) for shape, kind in outs],
        in_specs=specs,
        out_specs=[pl.BlockSpec(memory_space=pltpu.VMEM)] * len(outs),
        scratch_shapes=list(scratch),
        compiler_params=pltpu.CompilerParams(vmem_limit_bytes=vmem << 20),
        cost_estimate=pl.CostEstimate(flops=flops, bytes_accessed=1 << 20, transcendentals=0),
        name=name,
    )(*arguments)


def fast_device(
    dims, ids, counts, hash_scale, hash_shift, w_code, norm_gain, norm_bias, w_out, out_bias,
    cotangent,
):
    chips, reps, block, half = dims.chips, dims.reps, dims.block, dims.half
    dp, rep = lax.axis_index("dp"), lax.axis_index("rep")
    f32, bf16 = jnp.float32, jnp.bfloat16
    place, side = dp.reshape(1).astype(jnp.int32), rep.reshape(1).astype(jnp.int32)
    ids = ids.reshape(1, -1)
    scale_row, shift_row = hash_scale.reshape(1, -1), hash_shift.reshape(1, -1)
    gain_row, bias_row = norm_gain.reshape(1, -1), norm_bias.reshape(1, -1)
    kept = (scale_row, shift_row, w_code, gain_row, bias_row, w_out)
    loaded = (ids, scale_row, shift_row, w_code, cotangent, gain_row, bias_row, w_out)
    send, scale_row, shift_row, w_near, gain_row, bias_row, w_out_near = kernel_call(
        dims, first_kernel,
        [((dims.devices, dims.send_rows, LANES), bf16)]
        + [(x.shape, x.dtype) for x in kept],
        (counts, place, side) + tuple(pltpu.with_memory_space_constraint(x, pltpu.HBM) for x in loaded),
        3, "first", 10**9, hbm=range(3, 3 + len(loaded)),
        scratch=[pltpu.VMEM(x.shape, x.dtype) for x in (ids, cotangent)]
        + [pltpu.SemaphoreType.DMA((len(loaded),))],
    )
    recv = exchange(send)

    grads, stat, all_ids, all_counts = kernel_call(
        dims, middle_kernel,
        [
            ((chips, dims.grad_rows, LANES), bf16),
            ((8, half), f32),
            ((chips, dims.devices * dims.take), f32),
            ((dims.devices, LANES), f32),
        ],
        (
            place, side, recv, w_near, gain_row, bias_row, w_out_near, scale_row, shift_row,
        ),
        2,
        "middle", 10**9,
    )
    share = lax.all_to_all(grads, "dp", split_axis=0, concat_axis=0, tiled=True)

    def partner(x):
        return lax.ppermute(x, "rep", [(i, (i + 1) % reps) for i in range(reps)])

    w_own, stat, at, of = lax.optimization_barrier((w_code, stat, place, side))
    w_own = lax.dynamic_slice_in_dim(w_own, (at[0] * reps + of[0]) * block, block, 1)
    w_own = jnp.concatenate([w_own] * dims.groups, axis=1)
    packed = chips * dims.rows // dims.groups
    embedded, token = kernel_call(
        dims, embed_kernel, [((dims.slots, dims.width), bf16), ((8, LANES), f32)],
        (
            counts, side, ids, scale_row, shift_row,
            pltpu.with_memory_space_constraint(w_code, pltpu.HBM), stat, partner(stat),
            gain_row, bias_row,
            pltpu.with_memory_space_constraint(w_out, pltpu.HBM), out_bias.reshape(1, -1),
        ),
        2, "embed", 10**9, hbm=(5, 10),
        scratch=[
            pltpu.VMEM(w_code.shape, bf16), pltpu.VMEM(w_out.shape, bf16),
            pltpu.SemaphoreType.DMA((3,)),
        ],
    )
    fixed, *code = kernel_call(
        dims, owner_kernel,
        [((block + 8, dims.codes), f32)] + [((dims.piece, dims.codes), bf16)] * (dims.groups * dims.parts),
        (place, all_ids, all_counts, w_own, scale_row, shift_row, stat, token), 1,
        "owner", 4 * 10**9,
    )
    pair = share[:, dims.rows // dims.groups + block :, :]
    other = partner(pair)
    code_share, out_share = kernel_call(
        dims, last_kernel, [((block, dims.codes), f32), ((block, dims.width), f32)],
        (place, share, fixed, stat, *code), 1, "last", 10**9,
    )
    gain, bias = kernel_call(
        dims, join_kernel, [((1, dims.hidden), f32)] * 2, (side, pair, other), 1, "join", 10**6
    )
    return embedded, code_share, out_share, gain.reshape(-1), bias.reshape(-1)


def solution(mesh):
    rows = P(AXES)

    def per_device(*arguments):
        ids, w_code, w_out = arguments[0], arguments[4], arguments[7]
        dims = Dims(mesh, ids.shape[0], w_code.shape[0], w_code.shape[1], w_out.shape[1])
        if dims.reps == 2 and dims.fits():
            return fast_device(dims, *arguments)
        return general_device(*arguments)

    return jax.shard_map(
        per_device,
        mesh=mesh,
        in_specs=(rows, rows, P(), P(), P(), P(), P(), P(), P(), P(AXES, None)),
        out_specs=(P(AXES, None), P(AXES, None), P(AXES, None), P(), P()),
        check_vma=False,
    )
```
